32 devices in a mesh: orb: 16 (over z, y, core), grid: 2 (over x).
Axes of the slice: x: 2, y: 2, z: 4, core: 2. Of those that a mesh axis runs over, the one named last changes fastest.
Arguments:
- orbitals: bfloat16 [32, 11520], P('orb', 'grid'), may hold values from -1.5 to 1.5
- occupation: bfloat16 [32], P('orb'), may hold values from 0.29882812 to 1
Outputs:
- potentials: float32 [32, 11520], P('orb', 'grid')
- projectors: float32 [32, 11520], P('orb', 'grid')
The draws below stay inside these ranges and needn't reach their ends.
All inputs are finite; a program needn't handle non-finite values.
Results may differ from the reference program's by a relative error of at most 0.0025.
Values may be sent and summed in bfloat16 or wider, within the bound.
A program may use at most 64 MiB of HBM per device.

```python
import math
import jax
import jax.numpy as jnp
from jax import lax

NX = 20
NY = 24
NZ = 24
NORB = 32
NPTS = 11520


def shard_levels(rng, shape, split, smallest, top_value):
    def one(position, shards_of):
        heights = jax.random.uniform(jax.random.fold_in(jax.random.fold_in(rng, 6), position), (shards_of,), jnp.float32, smallest / len(split), top_value / len(split))
        return jnp.repeat(jnp.exp(heights), shape[position] // shards_of).reshape((-1,) + (1,) * (len(shape) - position - 1))

    factor_of = one(*split[0])
    for cut in split[1:]:
        factor_of = factor_of * one(*cut)
    return factor_of


def centred(own_key, extent, scale, bound, shards=(), held_as=jnp.bfloat16):
    array = jax.random.normal(own_key, extent, jnp.float32) * scale
    if len(shards) > 0:
        array = shard_levels(own_key, extent, shards, -0.22, 0.18) * array
    return jnp.clip(array, min=-bound, max=bound).astype(held_as)


def setup_inputs(seed: int = 0) -> dict:
    key_of = jax.random.split(jax.random.key(seed), 3)
    orbitals = centred(key_of[0], (NORB, NPTS), 0.25, 1.5, ((0, 16), (1, 2)))
    occupation = jnp.clip(0.29882812 + 0.7011719 * jax.random.uniform(key_of[1], (NORB,), jnp.float32) ** shard_levels(key_of[1], (NORB,), ((0, 16),), -0.2, 0.2), 0.29882812, 1.0).astype(jnp.bfloat16)
    return dict(orbitals=orbitals, occupation=occupation)


def hartley_table(length):
    index = jnp.arange(length, dtype=jnp.int32)
    product = index[:, None] * index[None, :] % length
    angle = 2.0 * math.pi / length * product.astype(jnp.float32)
    return (jnp.cos(angle) + jnp.sin(angle)).astype(jnp.bfloat16)

def signed_square(length):
    index = jnp.arange(length, dtype=jnp.int32)
    signed = jnp.where(index <= length // 2, index, index - length).astype(jnp.float32)
    return (2.0 * math.pi * signed / length) ** 2

def coulomb_kernel(size_x, size_y, size_z):
    total = signed_square(size_x)[:, None, None] + signed_square(size_y)[None, :, None] + signed_square(size_z)[None, None, :]
    safe = jnp.where(total > 0, total, 1.0)
    return jnp.where(total > 0, 1.0 / safe, 0.0) / (size_x * size_y * size_z)

def solve_pairs(density, table_x, table_y, table_z, kernel):
    fx = table_x.astype(jnp.float32)
    fy = table_y.astype(jnp.float32)
    fz = table_z.astype(jnp.float32)
    section = jnp.einsum('ax,pxyz->payz', fx, density.astype(jnp.float32)).astype(jnp.bfloat16)
    section = jnp.einsum('by,pxyz->pxbz', fy, section.astype(jnp.float32)).astype(jnp.bfloat16)
    spectrum = jnp.einsum('cz,pxyz->pxyc', fz, section.astype(jnp.float32))
    section = (spectrum * kernel).astype(jnp.bfloat16)
    section = jnp.einsum('cz,pxyz->pxyc', fz, section.astype(jnp.float32)).astype(jnp.bfloat16)
    section = jnp.einsum('by,pxyz->pxbz', fy, section.astype(jnp.float32)).astype(jnp.bfloat16)
    return jnp.einsum('ax,pxyz->payz', fx, section.astype(jnp.float32))

def reference(orbitals, occupation):
    table_x = hartley_table(NX)
    table_y = hartley_table(NY)
    table_z = hartley_table(NZ)
    kernel = coulomb_kernel(NX, NY, NZ)
    source = orbitals.astype(jnp.float32)
    weights = occupation.astype(jnp.float32)
    group = math.gcd(NORB, 32)
    blocks = source.reshape(NORB // group, group, NPTS)
    block_weights = weights.reshape(NORB // group, group)

    def potential_of(target):

        def accumulate(running, inputs):
            block, block_weight = inputs
            density = (target[None, :] * block).astype(jnp.bfloat16).reshape(group, NX, NY, NZ)
            potential = solve_pairs(density, table_x, table_y, table_z, kernel).reshape(group, NPTS)
            return (running - jnp.sum(block_weight[:, None] * potential * block, axis=0), None)
        running, unused = lax.scan(accumulate, jnp.zeros((NPTS,), jnp.float32), (blocks, block_weights))
        return running
    potentials = lax.map(potential_of, source)
    gram = lax.dot_general(source, potentials, (((1,), (1,)), ((), ())), precision=lax.Precision.HIGHEST) / NPTS
    factor = jnp.linalg.cholesky(-gram)
    inverse = lax.linalg.triangular_solve(factor, jnp.eye(NORB, dtype=jnp.float32), left_side=True, lower=True)
    projectors = jnp.dot(inverse, potentials, precision=lax.Precision.HIGHEST)
    return (potentials, projectors)
```

```python
import functools
import math

import jax
import jax.numpy as jnp
import numpy as np
from jax import lax
from jax.experimental import pallas as pl
from jax.experimental.pallas import tpu as pltpu
from jax.sharding import PartitionSpec as P

NX = 20
NY = 24
NZ = 24
NPTS = NX * NY * NZ
PLANE = NY * NZ
HALVES = 2
HX = NX // HALVES
ROWS = 16
BATCH = 8
MESH = pl.DeviceIdType.MESH


def hartley_table(length):
    index = np.arange(length, dtype=np.int32)
    product = index[:, None] * index[None, :] % length
    angle = np.float32(2.0 * math.pi / length) * product.astype(np.float32)
    return np.cos(angle) + np.sin(angle)


def signed_square(length):
    index = np.arange(length, dtype=np.int32)
    signed = np.where(index <= length // 2, index, index - length).astype(np.float32)
    return (np.float32(2.0 * math.pi) * signed / np.float32(length)) ** 2


def padded_rows(array):
    halves = array.reshape((HALVES, HX) + array.shape[1:])
    pad = [(0, 0), (0, ROWS - HX)] + [(0, 0)] * (array.ndim - 1)
    return np.pad(halves, pad).reshape((HALVES * ROWS,) + array.shape[1:])


def tables():
    table_x = padded_rows(padded_rows(hartley_table(NX)).T)
    table_x = np.kron(np.eye(BATCH, dtype=np.float32), table_x)
    table_y = np.kron(hartley_table(NY), np.eye(NZ, dtype=np.float32))
    table_z = np.kron(np.eye(16, dtype=np.float32), hartley_table(NZ))
    total = (
        signed_square(NX)[:, None, None]
        + signed_square(NY)[None, :, None]
        + signed_square(NZ)[None, None, :]
    )
    safe = np.where(total > 0, total, 1.0)
    kernel = np.where(total > 0, 1.0 / safe, 0.0) / NPTS
    kernel = padded_rows(kernel.reshape(NX, PLANE).astype(np.float32))
    return (
        jnp.asarray(table_x, jnp.bfloat16),
        jnp.asarray(table_y, jnp.bfloat16),
        jnp.asarray(table_z, jnp.bfloat16),
        jnp.asarray(kernel, jnp.float32),
    )


def column_of(matrix, k):
    if isinstance(k, int):
        return matrix[:, k : k + 1]
    lane = lax.broadcasted_iota(jnp.int32, matrix.shape, 1)
    return jnp.sum(jnp.where(lane == k, matrix, 0.0), axis=1, keepdims=True)


def row_of(matrix, k):
    if isinstance(k, int):
        return matrix[k : k + 1, :]
    line = lax.broadcasted_iota(jnp.int32, matrix.shape, 0)
    return jnp.sum(jnp.where(line == k, matrix, 0.0), axis=0, keepdims=True)


def loop(count, body, carry, most=64):
    if count <= most:
        for k in range(count):
            carry = body(k, carry)
        return carry
    return lax.fori_loop(0, count, body, carry)


def body(
    cols,
    own_ref,
    tx_ref,
    ty_ref,
    tz_ref,
    k_ref,
    pot_ref,
    proj_ref,
    src,
    part,
    part_in,
    pots,
    rowsum,
    gown,
    gall,
    gmat,
    s_a,
    s_y,
    s_c,
    s_x,
    s_cx,
    r_in,
    r_x,
    s_p,
    r_p,
    s_g,
    r_g,
    t_a,
    t_y,
    t_c,
    t_in,
):
    o = lax.axis_index("orb")
    g = lax.axis_index("grid")
    n_orb = 4 * cols
    n = 2 * n_orb
    r = o // 4
    y = (o % 4) // 2
    c = o % 2
    h = 1 - g
    f32 = jnp.float32
    o_y = r * 4 + (1 - y) * 2 + c
    o_c = r * 4 + y * 2 + (1 - c)

    barrier = pltpu.get_barrier_semaphore()

    @pl.loop(1, 2 * n_orb)
    def _(d):
        flat = (o * 2 + g + d) % (2 * n_orb)
        pl.semaphore_signal(
            barrier, inc=1, device_id=(flat // 2, flat % 2), device_id_type=MESH
        )

    pl.semaphore_wait(barrier, 2 * n_orb - 1)

    def copy(source, target, send, recv, orb, grid):
        return pltpu.make_async_remote_copy(
            src_ref=source,
            dst_ref=target,
            send_sem=send,
            recv_sem=recv,
            device_id=(orb, grid),
            device_id_type=MESH,
        )

    def to_column(d, source, target, send, recv):
        q = (r + d) % cols
        return copy(source, target, send.at[q], recv.at[r, y, c], q * 4 + y * 2 + c, g)

    @pl.loop(1, cols)
    def _(d):
        to_column(d, own_ref, src.at[r, y, c, g], s_a, r_in).start()

    copy(own_ref, src.at[r, y, c, g], s_y.at[r], r_in.at[r, y, c], o_y, g).start()
    copy(own_ref, src.at[r, y, c, g], s_x.at[r, y], r_x.at[r, y, c], o, h).start()
    copy(own_ref, src.at[r, y, c, g], s_c.at[r, y], r_in.at[r, y, c], o_c, g).start()
    src[r, y, c, g] = own_ref[...]

    def wait_block(ref, recv):
        copy(ref, ref, s_a.at[r], recv, o_c, g).wait_recv()

    def forward_x(q, u):
        return copy(
            src.at[q, u, c, g, h], src.at[q, u, c, g, h], s_x.at[q, u], r_x.at[q, u, c], o, h
        )

    def forward_c(q, u):
        return copy(
            src.at[q, u, c, g], src.at[q, u, c, g], s_c.at[q, u], r_in.at[q, u, c], o_c, g
        )

    def forward_y(q):
        return copy(src.at[q, y, c, g], src.at[q, y, c, g], s_y.at[q], r_in.at[q, y, c], o_y, g)

    def forward_cx(q, u):
        return copy(
            src.at[q, u, c, h, g], src.at[q, u, c, h, g], s_cx.at[q, u], r_x.at[q, u, c], o_c, g
        )

    @pl.loop(1, cols)
    def _(d):
        q = (r + d) % cols
        wait_block(src.at[q, y, c, g], r_in.at[q, y, c])
        forward_y(q).start()
        forward_x(q, y).start()
        forward_c(q, y).start()

    @pl.loop(0, cols)
    def _(d):
        q = (r + d) % cols
        wait_block(src.at[q, 1 - y, c, g], r_in.at[q, 1 - y, c])
        forward_x(q, 1 - y).start()
        forward_c(q, 1 - y).start()

    wait_block(src.at[r, y, c, h], r_x.at[r, y, c])
    forward_cx(r, y).start()

    @pl.loop(1, cols)
    def _(d):
        q = (r + d) % cols
        wait_block(src.at[q, y, c, h, g], r_x.at[q, y, c])
        forward_cx(q, y).start()

    @pl.loop(0, cols)
    def _(d):
        q = (r + d) % cols
        wait_block(src.at[q, 1 - y, c, h, g], r_x.at[q, 1 - y, c])
        forward_cx(q, 1 - y).start()

    tx = tx_ref[...]
    ty = ty_ref[...]
    tz = tz_ref[...]
    cut = tz.shape[0]
    rest = PLANE - cut
    kern = k_ref[...]

    def mm(a, b):
        return jnp.dot(a, b, preferred_element_type=f32)

    def along_z(a):
        return jnp.concatenate([mm(a[:, :cut], tz), mm(a[:, cut:], tz[:rest, :rest])], axis=1)

    per = BATCH // 2
    block = (BATCH, HALVES * ROWS, PLANE)
    flat_block = (BATCH * HALVES * ROWS, PLANE)

    def one_batch(core, step, first):
        raw = src[pl.ds(step * per, per), :, core, :, g].reshape(block).astype(f32)
        weight = raw[:, HX : HX + 1, :]
        for t in range(2):
            target = src[r, y, c, :, t].reshape(block[1:]).astype(f32)
            density = (raw * target[None]).astype(jnp.bfloat16).reshape(flat_block)
            s = mm(tx, density).astype(jnp.bfloat16)
            s = mm(s, ty).astype(jnp.bfloat16)
            s = along_z(s).reshape(block) * kern[None]
            s = along_z(s.reshape(flat_block).astype(jnp.bfloat16)).astype(jnp.bfloat16)
            s = mm(s, ty).astype(jnp.bfloat16)
            v = mm(tx, s).reshape(block)
            total = jnp.sum(weight * v * raw, axis=0).reshape(HALVES, ROWS, PLANE)
            if first:
                part[:, t] = -total
            else:
                part[:, t] -= total

    one_batch(c, 0, True)
    steps = cols // per
    if steps > 1:

        @pl.loop(1, steps)
        def _(k):
            one_batch(c, k, False)

    @pl.loop(0, cols)
    def _(q):
        for u in range(2):
            wait_block(src.at[q, u, 1 - c, g], r_in.at[q, u, 1 - c])
            wait_block(src.at[q, u, 1 - c, h, g], r_x.at[q, u, 1 - c])

    @pl.loop(0, steps)
    def _(k):
        one_batch(1 - c, k, False)

    swap = copy(part.at[h], part_in, s_p, r_p, o, h)
    swap.start()
    swap.wait_recv()
    final = part[g] + part_in[...]
    pot_ref[...] = final
    pots[r, y, c] = final

    @pl.loop(1, cols)
    def _(d):
        to_column(d, pot_ref, pots.at[r, y, c], t_a, t_in).start()

    copy(pot_ref, pots.at[r, y, c], t_y.at[r], t_in.at[r, y, c], o_y, g).start()
    copy(pot_ref, pots.at[r, y, c], t_c.at[r, y], t_in.at[r, y, c], o_c, g).start()

    @pl.loop(0, cols)
    def _(q):
        rows = src[q, :, :, g].reshape(8, ROWS, PLANE).astype(f32)
        for t in range(2):
            rowsum[t, pl.ds(pl.multiple_of(q * 8, 8), 8), :] = jnp.sum(
                rows * final[t][None], axis=1
            )

    ones = jnp.ones((8, PLANE), f32)

    def lane_sums(t):
        return lax.dot_general(
            ones,
            rowsum[t],
            (((1,), (1,)), ((), ())),
            precision=lax.Precision.HIGHEST,
            preferred_element_type=f32,
        )

    line = lax.broadcasted_iota(jnp.int32, (8, n), 0)
    gown[...] = jnp.where(line == 0, lane_sums(0), lane_sums(1))
    gall[g, o] = gown[...]

    def gram_to(d):
        flat = (o * 2 + g + d) % (2 * n_orb)
        return copy(gown, gall.at[g, o], s_g.at[d], r_g.at[g, o], flat // 2, flat % 2)

    @pl.loop(1, 2 * n_orb)
    def _(d):
        gram_to(d).start()

    def pass_y(q):
        return copy(pots.at[q, y, c], pots.at[q, y, c], t_y.at[q], t_in.at[q, y, c], o_y, g)

    def pass_c(q, u):
        return copy(pots.at[q, u, c], pots.at[q, u, c], t_c.at[q, u], t_in.at[q, u, c], o_c, g)

    @pl.loop(1, cols)
    def _(d):
        q = (r + d) % cols
        wait_block(pots.at[q, y, c], t_in.at[q, y, c])
        pass_y(q).start()
        pass_c(q, y).start()

    @pl.loop(1, 2 * n_orb)
    def _(d):
        flat = (o * 2 + g + d) % (2 * n_orb)
        wait_block(gall.at[flat % 2, flat // 2], r_g.at[flat % 2, flat // 2])

    @pl.loop(0, cols)
    def _(d):
        q = (r + d) % cols
        wait_block(pots.at[q, 1 - y, c], t_in.at[q, 1 - y, c])
        pass_c(q, 1 - y).start()

    def assemble(k, carry):
        pairs = [gall[0, 4 * k + j, 0:2, :] + gall[1, 4 * k + j, 0:2, :] for j in range(4)]
        start = 8 * k if isinstance(k, int) else pl.multiple_of(8 * k, 8)
        gmat[pl.ds(start, 8), :] = jnp.concatenate(pairs, axis=0)
        return carry

    loop(cols, assemble, 0, 16)
    gram = gmat[...]
    sym = (gram + gram.T) * f32(-0.5 / NPTS)
    row_id = lax.broadcasted_iota(jnp.int32, (n, n), 0)
    eye = (row_id == lax.broadcasted_iota(jnp.int32, (n, n), 1)).astype(f32)
    below = lax.broadcasted_iota(jnp.int32, (n, 1), 0)

    def eliminate(k, pair):
        left, right = pair
        row_l = row_of(left, k)
        scale = 1.0 / column_of(row_l, k)
        factor = jnp.where(below > k, column_of(left, k) * scale, 0.0)
        return left - factor * row_l, right - factor * row_of(right, k)

    left, right = loop(n, eliminate, (sym, eye))
    diag = jnp.sum(left * eye, axis=1, keepdims=True)
    inverse = right * (1.0 / jnp.sqrt(diag))
    a0, a1 = row_of(inverse, 2 * o), row_of(inverse, 2 * o + 1)

    @pl.loop(0, cols)
    def _(q):
        for u in range(2):
            wait_block(pots.at[q, u, 1 - c], t_in.at[q, u, 1 - c])

    def add(k, sums):
        p0, p1 = sums
        if isinstance(k, int):
            value = pots[k // 8, (k % 8) // 4, (k % 4) // 2, k % 2]
        else:
            value = pots[k // 8, lax.rem(k, 8) // 4, lax.rem(k, 4) // 2, lax.rem(k, 2)]
        return p0 + column_of(a0, k) * value, p1 + column_of(a1, k) * value

    zero = jnp.zeros((ROWS, PLANE), f32)
    p0, p1 = loop(n, add, (zero, zero))
    proj_ref[0] = p0
    proj_ref[1] = p1

    @pl.loop(1, cols)
    def _(d):
        to_column(d, own_ref, src.at[r, y, c, g], s_a, r_in).wait_send()
        to_column(d, pot_ref, pots.at[r, y, c], t_a, t_in).wait_send()
        q = (r + d) % cols
        forward_x(q, y).wait_send()

    copy(own_ref, src.at[r, y, c, g], s_x.at[r, y], r_x.at[r, y, c], o, h).wait_send()
    swap.wait_send()

    @pl.loop(0, cols)
    def _(q):
        forward_x(q, 1 - y).wait_send()
        forward_y(q).wait_send()
        pass_y(q).wait_send()
        for u in range(2):
            forward_c(q, u).wait_send()
            forward_cx(q, u).wait_send()
            pass_c(q, u).wait_send()

    @pl.loop(1, 2 * n_orb)
    def _(d):
        gram_to(d).wait_send()


def on_device(orbitals, occupation):
    n_orb = lax.axis_size("orb")
    cols = n_orb // 4
    n = 2 * n_orb
    own = orbitals.reshape(2, HX, PLANE)
    weight = jnp.broadcast_to(occupation[:, None, None], (2, 1, PLANE))
    fill = jnp.zeros((2, ROWS - HX - 1, PLANE), jnp.bfloat16)
    own = jnp.concatenate([own, weight, fill], axis=1)
    table_x, table_y, table_z, kernel = tables()
    f32 = jnp.float32
    dma = pltpu.SemaphoreType.DMA
    full = jax.ShapeDtypeStruct((2, ROWS, PLANE), f32)
    pot, proj = pl.pallas_call(
        functools.partial(body, cols),
        out_shape=(full, full),
        in_specs=[pl.BlockSpec(memory_space=pltpu.VMEM)] * 5,
        out_specs=[pl.BlockSpec(memory_space=pltpu.VMEM)] * 2,
        scratch_shapes=[
            pltpu.VMEM((cols, 2, 2, 2, 2, ROWS, PLANE), jnp.bfloat16),
            pltpu.VMEM((2, 2, ROWS, PLANE), f32),
            pltpu.VMEM((2, ROWS, PLANE), f32),
            pltpu.VMEM((cols, 2, 2, 2, ROWS, PLANE), f32),
            pltpu.VMEM((2, n, PLANE), f32),
            pltpu.VMEM((8, n), f32),
            pltpu.VMEM((2, n_orb, 8, n), f32),
            pltpu.VMEM((n, n), f32),
            dma((cols,)),
            dma((cols,)),
            dma((cols, 2)),
            dma((cols, 2)),
            dma((cols, 2)),
            dma((cols, 2, 2)),
            dma((cols, 2, 2)),
            dma,
            dma,
            dma((2 * n_orb,)),
            dma((2, n_orb)),
            dma((cols,)),
            dma((cols,)),
            dma((cols, 2)),
            dma((cols, 2, 2)),
        ],
        compiler_params=pltpu.CompilerParams(
            collective_id=0, has_side_effects=True, vmem_limit_bytes=60 * 1024 * 1024
        ),
        name="exchange",
    )(own, table_x, table_y, table_z, kernel)

    def flat(a):
        return a[:, :HX, :].reshape(2, HX * PLANE)

    return flat(pot), flat(proj)


def solution(mesh):
    return jax.shard_map(
        on_device,
        mesh=mesh,
        in_specs=(P("orb", "grid"), P("orb")),
        out_specs=(P("orb", "grid"), P("orb", "grid")),
        check_vma=False,
    )
```

```python
import functools
import math

import jax
import jax.numpy as jnp
import numpy as np
from jax import lax
from jax.experimental import pallas as pl
from jax.experimental.pallas import tpu as pltpu
from jax.sharding import PartitionSpec as P

NX = 20
NY = 24
NZ = 24
NPTS = NX * NY * NZ
PLANE = NY * NZ
HALVES = 2
HX = NX // HALVES
ROWS = 16
SENT = 12
BATCH = 8
MESH = pl.DeviceIdType.MESH


def hartley_table(length):
    index = np.arange(length, dtype=np.int32)
    product = index[:, None] * index[None, :] % length
    angle = np.float32(2.0 * math.pi / length) * product.astype(np.float32)
    return np.cos(angle) + np.sin(angle)


def signed_square(length):
    index = np.arange(length, dtype=np.int32)
    signed = np.where(index <= length // 2, index, index - length).astype(np.float32)
    return (np.float32(2.0 * math.pi) * signed / np.float32(length)) ** 2


def padded_rows(array):
    halves = array.reshape((HALVES, HX) + array.shape[1:])
    pad = [(0, 0), (0, ROWS - HX)] + [(0, 0)] * (array.ndim - 1)
    return np.pad(halves, pad).reshape((HALVES * ROWS,) + array.shape[1:])


def tables():
    table_x = padded_rows(padded_rows(hartley_table(NX)).T)
    table_x = np.kron(np.eye(BATCH, dtype=np.float32), table_x)
    table_y = np.kron(hartley_table(NY), np.eye(NZ, dtype=np.float32))
    table_z = np.kron(np.eye(16, dtype=np.float32), hartley_table(NZ))
    total = (
        signed_square(NX)[:, None, None]
        + signed_square(NY)[None, :, None]
        + signed_square(NZ)[None, None, :]
    )
    safe = np.where(total > 0, total, 1.0)
    kernel = np.where(total > 0, 1.0 / safe, 0.0) / NPTS
    kernel = padded_rows(kernel.reshape(NX, PLANE).astype(np.float32))
    return (
        jnp.asarray(table_x, jnp.bfloat16),
        jnp.asarray(table_y, jnp.bfloat16),
        jnp.asarray(table_z, jnp.bfloat16),
        jnp.asarray(kernel, jnp.float32),
    )


def column_of(matrix, k):
    if isinstance(k, int):
        return matrix[:, k : k + 1]
    lane = lax.broadcasted_iota(jnp.int32, matrix.shape, 1)
    return jnp.sum(jnp.where(lane == k, matrix, 0.0), axis=1, keepdims=True)


def row_of(matrix, k):
    if isinstance(k, int):
        return matrix[k : k + 1, :]
    line = lax.broadcasted_iota(jnp.int32, matrix.shape, 0)
    return jnp.sum(jnp.where(line == k, matrix, 0.0), axis=0, keepdims=True)


def loop(count, body, carry, most=64):
    if count <= most:
        for k in range(count):
            carry = body(k, carry)
        return carry
    return lax.fori_loop(0, count, body, carry)


def body(
    cols,
    own_ref,
    occ_ref,
    tx_hbm,
    ty_hbm,
    tz_hbm,
    k_hbm,
    pot_ref,
    proj_ref,
    tx_ref,
    ty_ref,
    tz_ref,
    k_ref,
    src,
    part,
    part_in,
    pots,
    rowsum,
    gown,
    gall,
    gmat,
    s_tab,
    s_x,
    r_x,
    s_a,
    s_y,
    s_c,
    r_in,
    s_p,
    r_p,
    s_g,
    r_g,
    t_a,
    t_y,
    t_c,
    t_in,
):
    o = lax.axis_index("orb")
    g = lax.axis_index("grid")
    n_orb = 4 * cols
    n = 2 * n_orb
    r = o // 4
    y = (o % 4) // 2
    c = o % 2
    h = 1 - g
    f32 = jnp.float32
    bf16 = jnp.bfloat16
    o_y = r * 4 + (1 - y) * 2 + c
    o_c = r * 4 + y * 2 + (1 - c)

    loads = [
        pltpu.make_async_copy(a, b, s_tab.at[i])
        for i, (a, b) in enumerate(
            ((tx_hbm, tx_ref), (ty_hbm, ty_ref), (tz_hbm, tz_ref), (k_hbm, k_ref))
        )
    ]
    for load in loads:
        load.start()

    barrier = pltpu.get_barrier_semaphore()

    @pl.loop(1, 2 * n_orb)
    def _(d):
        flat = (o * 2 + g + d) % (2 * n_orb)
        pl.semaphore_signal(
            barrier, inc=1, device_id=(flat // 2, flat % 2), device_id_type=MESH
        )

    own = own_ref[...].astype(f32)
    occ = occ_ref[...].astype(f32)
    for t in range(2):
        lines = [own[t : t + 1, PLANE * x : PLANE * (x + 1)] for x in range(HX)]
        lines.append(jnp.broadcast_to(occ[:, t : t + 1], (1, PLANE)))
        lines.append(jnp.zeros((SENT - HX - 1, PLANE), f32))
        src[r, y, c, g, t] = jnp.concatenate(lines, axis=0).astype(bf16)

    pl.semaphore_wait(barrier, 2 * n_orb - 1)

    def copy(source, target, send, recv, orb, grid):
        return pltpu.make_async_remote_copy(
            src_ref=source,
            dst_ref=target,
            send_sem=send,
            recv_sem=recv,
            device_id=(orb, grid),
            device_id_type=MESH,
        )

    def piece(j, q, u, w):
        half = h if j == 1 else g
        t = h if j == 2 else g
        return src.at[q, u, w, half, t]

    def same(ref, send, recv, orb):
        return copy(ref, ref, send, recv, orb, g)

    def to_column(j, d):
        q = (r + d) % cols
        return same(piece(j, r, y, c), s_a.at[j, q], r_in.at[j, r, y, c], q * 4 + y * 2 + c)

    def to_y(j, q):
        return same(piece(j, q, y, c), s_y.at[j, q], r_in.at[j, q, y, c], o_y)

    def to_core(j, q, u):
        return same(piece(j, q, u, c), s_c.at[j, q, u], r_in.at[j, q, u, c], o_c)

    def arrived(j, q, u, w):
        same(piece(j, q, u, w), s_a.at[j, r], r_in.at[j, q, u, w], o_c).wait_recv()

    own_block = src.at[r, y, c, g]
    cross = copy(own_block, own_block, s_x, r_x, o, h)
    other_block = src.at[r, y, c, h]
    cross_in = copy(other_block, other_block, s_x, r_x, o, h)
    cross.start()

    def send_own(j):
        @pl.loop(1, cols)
        def _(d):
            to_column(j, cols - d).start()

        to_y(j, r).start()
        to_core(j, r, y).start()

    send_own(0)
    cross_in.wait_recv()
    send_own(1)

    def relay_column(j):
        @pl.loop(1, cols)
        def _(d):
            q = (r + d) % cols
            arrived(j, q, y, c)
            to_y(j, q).start()
            to_core(j, q, y).start()

    def relay_y(j):
        @pl.loop(0, cols)
        def _(d):
            q = (r + d) % cols
            arrived(j, q, 1 - y, c)
            to_core(j, q, 1 - y).start()

    def other_core(j, u):
        @pl.loop(0, cols)
        def _(q):
            arrived(j, q, u, 1 - c)

    relay_column(0)
    relay_column(1)
    send_own(2)
    for load in loads:
        load.wait()
    other_core(0, y)
    other_core(1, y)

    tx = tx_ref[...]
    ty = ty_ref[...]
    tz = tz_ref[...]
    cut = tz.shape[0]
    rest = PLANE - cut
    kern = k_ref[...]

    def mm(a, b):
        return jnp.dot(a, b, preferred_element_type=f32)

    def along_z(a):
        return jnp.concatenate([mm(a[:, :cut], tz), mm(a[:, cut:], tz[:rest, :rest])], axis=1)

    per = BATCH // 2
    block = (BATCH, HALVES * ROWS, PLANE)
    flat_block = (BATCH * HALVES * ROWS, PLANE)
    steps = cols // per
    thin = (BATCH * HALVES, SENT, PLANE)

    def whole(a):
        a = a.astype(f32)
        if SENT == ROWS:
            return a
        fill = jnp.zeros((a.shape[0], ROWS - SENT, PLANE), f32)
        return jnp.concatenate([a, fill], axis=1)

    def one_batch(u, step, t, first):
        raw = whole(src[pl.ds(step * per, per), u, :, :, g].reshape(thin)).reshape(block)
        weight = raw[:, HX : HX + 1, :]
        target = whole(src[r, y, c, :, t]).reshape(block[1:])
        density = (raw * target[None]).astype(bf16).reshape(flat_block)
        s = mm(tx, density).astype(bf16)
        s = mm(s, ty).astype(bf16)
        s = along_z(s).reshape(block) * kern[None]
        s = along_z(s.reshape(flat_block).astype(bf16)).astype(bf16)
        s = mm(s, ty).astype(bf16)
        v = mm(tx, s).reshape(block)
        total = jnp.sum(weight * v * raw, axis=0).reshape(HALVES, ROWS, PLANE)[:, :HX]
        if first:
            part[:, t] = -total
        else:
            part[:, t] -= total

    def batches(u, t, first):
        if first:
            one_batch(u, 0, t, True)
        if steps > int(first):

            @pl.loop(int(first), steps)
            def _(k):
                one_batch(u, k, t, False)

    batches(y, 0, True)
    relay_y(0)
    relay_y(1)
    batches(y, 1, True)
    relay_column(2)
    other_core(0, 1 - y)
    other_core(1, 1 - y)
    batches(1 - y, 0, False)

    def swap(t):
        return copy(part.at[h, t], part_in.at[t], s_p.at[t], r_p.at[t], o, h)

    swap(0).start()
    relay_y(2)
    batches(1 - y, 1, False)
    swap(1).start()

    other_core(2, y)
    other_core(2, 1 - y)

    def pot_at(t, q, u, w):
        return pots.at[q, u, w, t]

    def pot_column(t, d):
        q = (r + d) % cols
        return same(pot_at(t, r, y, c), t_a.at[t, q], t_in.at[t, r, y, c], q * 4 + y * 2 + c)

    def pot_y(t, q):
        return same(pot_at(t, q, y, c), t_y.at[t, q], t_in.at[t, q, y, c], o_y)

    def pot_core(t, q, u):
        return same(pot_at(t, q, u, c), t_c.at[t, q, u], t_in.at[t, q, u, c], o_c)

    def pot_arrived(t, q, u, w):
        same(pot_at(t, q, u, w), t_a.at[t, r], t_in.at[t, q, u, w], o_c).wait_recv()

    def send_pots(t):
        @pl.loop(1, cols)
        def _(d):
            pot_column(t, cols - d).start()

        pot_y(t, r).start()
        pot_core(t, r, y).start()

    def gram_rows(t, value):
        @pl.loop(0, cols)
        def _(q):
            rows = src[q, :, :, g].reshape(8, SENT, PLANE).astype(f32)[:, :HX]
            rowsum[t, pl.ds(pl.multiple_of(q * 8, 8), 8), :] = jnp.sum(rows * value[None], axis=1)

        ones = jnp.ones((8, PLANE), f32)
        sums = lax.dot_general(
            ones,
            rowsum[t],
            (((1,), (1,)), ((), ())),
            precision=lax.Precision.HIGHEST,
            preferred_element_type=f32,
        )
        gown[t : t + 1, :] = sums[0:1]

    def finish(t):
        swap(t).wait_recv()
        value = part[g, t] + part_in[t]
        pots[r, y, c, t] = value
        return value

    value0 = finish(0)
    send_pots(0)
    gram_rows(0, value0)
    value1 = finish(1)
    gram_rows(1, value1)
    gall[g, o] = gown[...]

    def gram_to(d):
        flat = (o * 2 + g + d) % (2 * n_orb)
        return copy(gown, gall.at[g, o], s_g.at[d], r_g.at[g, o], flat // 2, flat % 2)

    @pl.loop(1, 2 * n_orb)
    def _(d):
        gram_to(d).start()

    send_pots(1)

    def write(ref, t, value):
        for x in range(0, HX, 2):
            pair = jnp.concatenate([value[x : x + 1], value[x + 1 : x + 2]], axis=1)
            ref[t : t + 1, PLANE * x : PLANE * (x + 2)] = pair

    write(pot_ref, 0, value0)
    write(pot_ref, 1, value1)

    def pot_relay_column(t):
        @pl.loop(1, cols)
        def _(d):
            q = (r + d) % cols
            pot_arrived(t, q, y, c)
            pot_y(t, q).start()
            pot_core(t, q, y).start()

    def pot_relay_y(t):
        @pl.loop(0, cols)
        def _(d):
            q = (r + d) % cols
            pot_arrived(t, q, 1 - y, c)
            pot_core(t, q, 1 - y).start()

    pot_relay_column(0)

    @pl.loop(1, 2 * n_orb)
    def _(d):
        flat = (o * 2 + g + d) % (2 * n_orb)
        there = gall.at[flat % 2, flat // 2]
        copy(there, there, s_g.at[0], r_g.at[flat % 2, flat // 2], o_c, g).wait_recv()

    pot_relay_column(1)
    pot_relay_y(0)

    def assemble(k, carry):
        pairs = [gall[0, 4 * k + j] + gall[1, 4 * k + j] for j in range(4)]
        start = 8 * k if isinstance(k, int) else pl.multiple_of(8 * k, 8)
        gmat[pl.ds(start, 8), :] = jnp.concatenate(pairs, axis=0)
        return carry

    loop(cols, assemble, 0, 16)
    gram = gmat[...]
    sym = (gram + gram.T) * f32(-0.5 / NPTS)
    row_id = lax.broadcasted_iota(jnp.int32, (n, n), 0)
    eye = (row_id == lax.broadcasted_iota(jnp.int32, (n, n), 1)).astype(f32)
    below = lax.broadcasted_iota(jnp.int32, (n, 1), 0)

    def eliminate(k, pair):
        left, right = pair
        row_l = row_of(left, k)
        scale = 1.0 / column_of(row_l, k)
        factor = jnp.where(below > k, column_of(left, k) * scale, 0.0)
        return left - factor * row_l, right - factor * row_of(right, k)

    left, right = loop(n, eliminate, (sym, eye))
    diag = jnp.sum(left * eye, axis=1, keepdims=True)
    inverse = right * (1.0 / jnp.sqrt(diag))
    a0, a1 = row_of(inverse, 2 * o), row_of(inverse, 2 * o + 1)

    pot_relay_y(1)

    @pl.loop(0, cols)
    def _(q):
        for u in range(2):
            for t in range(2):
                pot_arrived(t, q, u, 1 - c)

    def add(k, sums):
        p0, p1 = sums
        if isinstance(k, int):
            value = pots[k // 8, (k % 8) // 4, (k % 4) // 2, k % 2]
        else:
            value = pots[k // 8, lax.rem(k, 8) // 4, lax.rem(k, 4) // 2, lax.rem(k, 2)]
        return p0 + column_of(a0, k) * value, p1 + column_of(a1, k) * value

    zero = jnp.zeros((HX, PLANE), f32)
    p0, p1 = loop(n, add, (zero, zero))
    write(proj_ref, 0, p0)
    write(proj_ref, 1, p1)

    cross.wait_send()
    for t in range(2):
        swap(t).wait_send()

    @pl.loop(1, cols)
    def _(d):
        for j in range(3):
            to_column(j, d).wait_send()
        for t in range(2):
            pot_column(t, d).wait_send()

    @pl.loop(0, cols)
    def _(q):
        for j in range(3):
            to_y(j, q).wait_send()
            for u in range(2):
                to_core(j, q, u).wait_send()
        for t in range(2):
            pot_y(t, q).wait_send()
            for u in range(2):
                pot_core(t, q, u).wait_send()

    @pl.loop(1, 2 * n_orb)
    def _(d):
        gram_to(d).wait_send()


def on_device(orbitals, occupation):
    n_orb = lax.axis_size("orb")
    cols = n_orb // 4
    n = 2 * n_orb
    consts = tables()
    f32 = jnp.float32
    bf16 = jnp.bfloat16
    dma = pltpu.SemaphoreType.DMA
    vmem = pl.BlockSpec(memory_space=pltpu.VMEM)
    full = jax.ShapeDtypeStruct(orbitals.shape, f32)
    return pl.pallas_call(
        functools.partial(body, cols),
        out_shape=(full, full),
        in_specs=[vmem] * 2 + [pl.BlockSpec(memory_space=pl.ANY)] * 4,
        out_specs=(vmem, vmem),
        scratch_shapes=[
            *[pltpu.VMEM(a.shape, a.dtype) for a in consts],
            pltpu.VMEM((cols, 2, 2, 2, 2, SENT, PLANE), bf16),
            pltpu.VMEM((2, 2, HX, PLANE), f32),
            pltpu.VMEM((2, HX, PLANE), f32),
            pltpu.VMEM((cols, 2, 2, 2, HX, PLANE), f32),
            pltpu.VMEM((2, n, PLANE), f32),
            pltpu.VMEM((2, n), f32),
            pltpu.VMEM((2, n_orb, 2, n), f32),
            pltpu.VMEM((n, n), f32),
            dma((4,)),
            dma,
            dma,
            dma((3, cols)),
            dma((3, cols)),
            dma((3, cols, 2)),
            dma((3, cols, 2, 2)),
            dma((2,)),
            dma((2,)),
            dma((2 * n_orb,)),
            dma((2, n_orb)),
            dma((2, cols)),
            dma((2, cols)),
            dma((2, cols, 2)),
            dma((2, cols, 2, 2)),
        ],
        compiler_params=pltpu.CompilerParams(
            collective_id=0, has_side_effects=True, vmem_limit_bytes=60 * 1024 * 1024
        ),
        name="exchange",
    )(orbitals, occupation[None], *consts)


def solution(mesh):
    return jax.shard_map(
        on_device,
        mesh=mesh,
        in_specs=(P("orb", "grid"), P("orb")),
        out_specs=(P("orb", "grid"), P("orb", "grid")),
        check_vma=False,
    )
```

```python
import functools
import math

import jax
import jax.numpy as jnp
import numpy as np
from jax import lax
from jax.experimental import pallas as pl
from jax.experimental.pallas import tpu as pltpu
from jax.sharding import PartitionSpec as P

NX = 20
NY = 24
NZ = 24
NPTS = NX * NY * NZ
PLANE = NY * NZ
HALVES = 2
HX = NX // HALVES
ROWS = 16
SENT = 12
LANES = 128
BATCH = 8
MESH = pl.DeviceIdType.MESH


def hartley_table(length):
    index = np.arange(length, dtype=np.int32)
    product = index[:, None] * index[None, :] % length
    angle = np.float32(2.0 * math.pi / length) * product.astype(np.float32)
    return np.cos(angle) + np.sin(angle)


def signed_square(length):
    index = np.arange(length, dtype=np.int32)
    signed = np.where(index <= length // 2, index, index - length).astype(np.float32)
    return (np.float32(2.0 * math.pi) * signed / np.float32(length)) ** 2


def padded_rows(array):
    halves = array.reshape((HALVES, HX) + array.shape[1:])
    pad = [(0, 0), (0, ROWS - HX)] + [(0, 0)] * (array.ndim - 1)
    return np.pad(halves, pad).reshape((HALVES * ROWS,) + array.shape[1:])


def tables():
    table_x = padded_rows(padded_rows(hartley_table(NX)).T)
    table_x = np.kron(np.eye(BATCH, dtype=np.float32), table_x)
    table_y = np.kron(hartley_table(NY), np.eye(NZ, dtype=np.float32))
    table_z = np.kron(np.eye(16, dtype=np.float32), hartley_table(NZ))
    total = (
        signed_square(NX)[:, None, None]
        + signed_square(NY)[None, :, None]
        + signed_square(NZ)[None, None, :]
    )
    safe = np.where(total > 0, total, 1.0)
    kernel = np.where(total > 0, 1.0 / safe, 0.0) / NPTS
    kernel = padded_rows(kernel.reshape(NX, PLANE).astype(np.float32))
    return (
        jnp.asarray(table_x, jnp.bfloat16),
        jnp.asarray(table_y, jnp.bfloat16),
        jnp.asarray(table_z, jnp.bfloat16),
        jnp.asarray(kernel, jnp.float32),
    )


def column_of(matrix, k):
    if isinstance(k, int):
        return matrix[:, k : k + 1]
    lane = lax.broadcasted_iota(jnp.int32, matrix.shape, 1)
    return jnp.sum(jnp.where(lane == k, matrix, 0.0), axis=1, keepdims=True)


def row_of(matrix, k):
    if isinstance(k, int):
        return matrix[k : k + 1, :]
    line = lax.broadcasted_iota(jnp.int32, matrix.shape, 0)
    return jnp.sum(jnp.where(line == k, matrix, 0.0), axis=0, keepdims=True)


def loop(count, body, carry, most=64):
    if count <= most:
        for k in range(count):
            carry = body(k, carry)
        return carry
    return lax.fori_loop(0, count, body, carry)


def body(
    cols,
    own_ref,
    occ_ref,
    tx_hbm,
    ty_hbm,
    tz_hbm,
    k_hbm,
    pot_ref,
    proj_ref,
    tx_ref,
    ty_ref,
    tz_ref,
    k_ref,
    src,
    part,
    part_in,
    pots,
    rowsum,
    gown,
    gall,
    gmat,
    s_tab,
    s_x,
    r_x,
    s_a,
    s_y,
    s_c,
    r_in,
    s_p,
    r_p,
    s_g,
    r_g,
    t_a,
    t_y,
    t_c,
    t_in,
):
    o = lax.axis_index("orb")
    g = lax.axis_index("grid")
    n_orb = 4 * cols
    n = 2 * n_orb
    r = o // 4
    y = (o % 4) // 2
    c = o % 2
    h = 1 - g
    f32 = jnp.float32
    bf16 = jnp.bfloat16
    o_y = r * 4 + (1 - y) * 2 + c
    o_c = r * 4 + y * 2 + (1 - c)

    loads = [
        pltpu.make_async_copy(a, b, s_tab.at[i])
        for i, (a, b) in enumerate(
            ((tx_hbm, tx_ref), (ty_hbm, ty_ref), (tz_hbm, tz_ref), (k_hbm, k_ref))
        )
    ]
    for load in loads:
        load.start()

    barrier = pltpu.get_barrier_semaphore()

    def greet(orb, grid):
        pl.semaphore_signal(barrier, inc=1, device_id=(orb, grid), device_id_type=MESH)

    @pl.loop(1, cols)
    def _(d):
        greet((r + d) % cols * 4 + y * 2 + c, g)

    greet(o, h)
    greet(o_y, g)
    greet(o_c, g)

    own = own_ref[...].astype(f32)
    occ = occ_ref[...].astype(f32)
    for t in range(2):
        lines = [own[t : t + 1, PLANE * x : PLANE * (x + 1)] for x in range(HX)]
        lines.append(jnp.broadcast_to(occ[:, t : t + 1], (1, PLANE)))
        lines.append(jnp.zeros((SENT - HX - 1, PLANE), f32))
        src[r, y, c, g, t] = jnp.concatenate(lines, axis=0).astype(bf16)

    pl.semaphore_wait(barrier, cols + 2)

    def copy(source, target, send, recv, orb, grid):
        return pltpu.make_async_remote_copy(
            src_ref=source,
            dst_ref=target,
            send_sem=send,
            recv_sem=recv,
            device_id=(orb, grid),
            device_id_type=MESH,
        )

    def piece(j, q, u, w):
        half = h if j == 1 else g
        t = h if j == 2 else g
        return src.at[q, u, w, half, t]

    def same(ref, send, recv, orb):
        return copy(ref, ref, send, recv, orb, g)

    def to_column(j, d):
        q = (r + d) % cols
        return same(piece(j, r, y, c), s_a.at[j, q], r_in.at[j, r, y, c], q * 4 + y * 2 + c)

    def to_y(j, q):
        return same(piece(j, q, y, c), s_y.at[j, q], r_in.at[j, q, y, c], o_y)

    def to_core(j, q, u):
        return same(piece(j, q, u, c), s_c.at[j, q, u], r_in.at[j, q, u, c], o_c)

    def arrived(j, q, u, w):
        same(piece(j, q, u, w), s_a.at[j, r], r_in.at[j, q, u, w], o_c).wait_recv()

    own_block = src.at[r, y, c, g]
    cross = copy(own_block, own_block, s_x, r_x, o, h)
    other_block = src.at[r, y, c, h]
    cross_in = copy(other_block, other_block, s_x, r_x, o, h)
    cross.start()

    def send_own(j):
        @pl.loop(1, cols)
        def _(d):
            to_column(j, cols - d).start()

        to_y(j, r).start()
        to_core(j, r, y).start()

    send_own(0)
    cross_in.wait_recv()
    send_own(1)

    def relay_column(j):
        @pl.loop(1, cols)
        def _(d):
            q = (r + d) % cols
            arrived(j, q, y, c)
            to_y(j, q).start()
            to_core(j, q, y).start()

    def relay_y(j):
        @pl.loop(0, cols)
        def _(d):
            q = (r + d) % cols
            arrived(j, q, 1 - y, c)
            to_core(j, q, 1 - y).start()

    def other_core(j, u):
        @pl.loop(0, cols)
        def _(q):
            arrived(j, q, u, 1 - c)

    relay_column(0)
    relay_column(1)
    send_own(2)
    for load in loads:
        load.wait()
    other_core(0, y)
    other_core(1, y)

    tx = tx_ref[...]
    ty = ty_ref[...]
    tz = tz_ref[...]
    cut = tz.shape[0]
    rest = PLANE - cut
    kern = k_ref[...]

    def mm(a, b):
        return jnp.dot(a, b, preferred_element_type=f32)

    def along_z(a):
        return jnp.concatenate([mm(a[:, :cut], tz), mm(a[:, cut:], tz[:rest, :rest])], axis=1)

    per = BATCH // 2
    block = (BATCH, HALVES * ROWS, PLANE)
    flat_block = (BATCH * HALVES * ROWS, PLANE)
    steps = cols // per
    thin = (BATCH * HALVES, SENT, PLANE)

    def whole(a):
        a = a.astype(f32)
        if SENT == ROWS:
            return a
        fill = jnp.zeros((a.shape[0], ROWS - SENT, PLANE), f32)
        return jnp.concatenate([a, fill], axis=1)

    def one_batch(u, step, t, first):
        raw = whole(src[pl.ds(step * per, per), u, :, :, g].reshape(thin)).reshape(block)
        weight = raw[:, HX : HX + 1, :]
        target = whole(src[r, y, c, :, t]).reshape(block[1:])
        density = (raw * target[None]).astype(bf16).reshape(flat_block)
        s = mm(tx, density).astype(bf16)
        s = mm(s, ty).astype(bf16)
        s = along_z(s).reshape(block) * kern[None]
        s = along_z(s.reshape(flat_block).astype(bf16)).astype(bf16)
        s = mm(s, ty).astype(bf16)
        v = mm(tx, s).reshape(block)
        total = jnp.sum(weight * v * raw, axis=0).reshape(HALVES, ROWS, PLANE)[:, :HX]
        if first:
            part[:, t] = -total
        else:
            part[:, t] -= total

    def batches(u, t, first):
        if first:
            one_batch(u, 0, t, True)
        if steps > int(first):

            @pl.loop(int(first), steps)
            def _(k):
                one_batch(u, k, t, False)

    batches(y, 0, True)
    relay_y(0)
    relay_y(1)
    batches(y, 1, True)
    relay_column(2)
    other_core(0, 1 - y)
    other_core(1, 1 - y)
    batches(1 - y, 0, False)

    def swap(t):
        return copy(part.at[h, t], part_in.at[t], s_p.at[t], r_p.at[t], o, h)

    swap(0).start()
    batches(1 - y, 1, False)
    swap(1).start()

    relay_y(2)

    def pot_at(t, q, u, w):
        return pots.at[q, u, w, t]

    def pot_column(t, d):
        q = (r + d) % cols
        return same(pot_at(t, r, y, c), t_a.at[t, q], t_in.at[t, r, y, c], q * 4 + y * 2 + c)

    def pot_y(t, q):
        return same(pot_at(t, q, y, c), t_y.at[t, q], t_in.at[t, q, y, c], o_y)

    def pot_core(t, q, u):
        return same(pot_at(t, q, u, c), t_c.at[t, q, u], t_in.at[t, q, u, c], o_c)

    def pot_arrived(t, q, u, w):
        same(pot_at(t, q, u, w), t_a.at[t, r], t_in.at[t, q, u, w], o_c).wait_recv()

    def send_pots(t):
        @pl.loop(1, cols)
        def _(d):
            pot_column(t, cols - d).start()

        pot_y(t, r).start()
        pot_core(t, r, y).start()

    def gram_rows(t, value):
        @pl.loop(0, cols)
        def _(q):
            rows = src[q, :, :, g].reshape(8, SENT, PLANE).astype(f32)[:, :HX]
            sums = jnp.sum(rows * value[None], axis=1)
            fold = sums[:, :LANES]
            for k in range(LANES, PLANE - LANES + 1, LANES):
                fold += sums[:, k : k + LANES]
            tail = PLANE % LANES
            if tail:
                last = jnp.zeros((8, LANES - tail), f32)
                fold += jnp.concatenate([sums[:, PLANE - tail :], last], axis=1)
            rowsum[t, pl.ds(pl.multiple_of(q * 8, 8), 8), :] = fold

        ones = jnp.ones((8, LANES), f32)
        sums = lax.dot_general(
            ones,
            rowsum[t],
            (((1,), (1,)), ((), ())),
            precision=lax.Precision.HIGHEST,
            preferred_element_type=f32,
        )
        gown[t : t + 1, :] = sums[0:1]

    def finish(t):
        swap(t).wait_recv()
        value = part[g, t] + part_in[t]
        pots[r, y, c, t] = value
        return value

    value0 = finish(0)
    send_pots(0)
    other_core(2, y)
    other_core(2, 1 - y)
    gram_rows(0, value0)
    value1 = finish(1)
    gram_rows(1, value1)
    gall[g, o] = gown[...]

    def gram_to(d):
        flat = (o * 2 + g + d) % (2 * n_orb)
        return copy(gown, gall.at[g, o], s_g.at[d], r_g.at[g, o], flat // 2, flat % 2)

    @pl.loop(1, 2 * n_orb)
    def _(d):
        gram_to(d).start()

    send_pots(1)

    def write(ref, t, value):
        for x in range(0, HX, 2):
            pair = jnp.concatenate([value[x : x + 1], value[x + 1 : x + 2]], axis=1)
            ref[t : t + 1, PLANE * x : PLANE * (x + 2)] = pair

    write(pot_ref, 0, value0)
    write(pot_ref, 1, value1)

    def pot_relay_column(t):
        @pl.loop(1, cols)
        def _(d):
            q = (r + d) % cols
            pot_arrived(t, q, y, c)
            pot_y(t, q).start()
            pot_core(t, q, y).start()

    def pot_relay_y(t):
        @pl.loop(0, cols)
        def _(d):
            q = (r + d) % cols
            pot_arrived(t, q, 1 - y, c)
            pot_core(t, q, 1 - y).start()

    pot_relay_column(0)
    pot_relay_column(1)
    pot_relay_y(0)

    cross.wait_send()
    for t in range(2):
        swap(t).wait_send()

    @pl.loop(1, cols)
    def _(d):
        for j in range(3):
            to_column(j, d).wait_send()

    @pl.loop(0, cols)
    def _(q):
        for j in range(3):
            to_y(j, q).wait_send()
            for u in range(2):
                to_core(j, q, u).wait_send()

    @pl.loop(1, 2 * n_orb)
    def _(d):
        flat = (o * 2 + g + d) % (2 * n_orb)
        there = gall.at[flat % 2, flat // 2]
        copy(there, there, s_g.at[0], r_g.at[flat % 2, flat // 2], o_c, g).wait_recv()

    def assemble(k, carry):
        pairs = [gall[0, 4 * k + j] + gall[1, 4 * k + j] for j in range(4)]
        start = 8 * k if isinstance(k, int) else pl.multiple_of(8 * k, 8)
        gmat[pl.ds(start, 8), :] = jnp.concatenate(pairs, axis=0)
        return carry

    loop(cols, assemble, 0, 16)
    gram = gmat[...]
    sym = (gram + gram.T) * f32(-0.5 / NPTS)
    row_id = lax.broadcasted_iota(jnp.int32, (n, n), 0)
    eye = (row_id == lax.broadcasted_iota(jnp.int32, (n, n), 1)).astype(f32)
    below = lax.broadcasted_iota(jnp.int32, (n, 1), 0)

    def eliminate(k, pair):
        left, right = pair
        row_l = row_of(left, k)
        scale = 1.0 / column_of(row_l, k)
        factor = jnp.where(below > k, column_of(left, k) * scale, 0.0)
        return left - factor * row_l, right - factor * row_of(right, k)

    early = n * 3 // 4
    if n <= 64:
        pair = loop(early, eliminate, (sym, eye))
        pot_relay_y(1)
        for k in range(early, n):
            pair = eliminate(k, pair)
        left, right = pair
    else:
        pot_relay_y(1)
        left, right = loop(n, eliminate, (sym, eye))
    diag = jnp.sum(left * eye, axis=1, keepdims=True)
    inverse = right * (1.0 / jnp.sqrt(diag))
    a0, a1 = row_of(inverse, 2 * o), row_of(inverse, 2 * o + 1)

    @pl.loop(0, cols)
    def _(q):
        for u in range(2):
            for t in range(2):
                pot_arrived(t, q, u, 1 - c)

    def add(k, sums):
        p0, p1 = sums
        if isinstance(k, int):
            value = pots[k // 8, (k % 8) // 4, (k % 4) // 2, k % 2]
        else:
            value = pots[k // 8, lax.rem(k, 8) // 4, lax.rem(k, 4) // 2, lax.rem(k, 2)]
        return p0 + column_of(a0, k) * value, p1 + column_of(a1, k) * value

    zero = jnp.zeros((HX, PLANE), f32)
    p0, p1 = loop(n, add, (zero, zero))
    write(proj_ref, 0, p0)
    write(proj_ref, 1, p1)

    @pl.loop(1, cols)
    def _(d):
        for t in range(2):
            pot_column(t, d).wait_send()

    @pl.loop(0, cols)
    def _(q):
        for t in range(2):
            pot_y(t, q).wait_send()
            for u in range(2):
                pot_core(t, q, u).wait_send()

    @pl.loop(1, 2 * n_orb)
    def _(d):
        gram_to(d).wait_send()


def on_device(orbitals, occupation):
    n_orb = lax.axis_size("orb")
    cols = n_orb // 4
    n = 2 * n_orb
    consts = tables()
    f32 = jnp.float32
    bf16 = jnp.bfloat16
    dma = pltpu.SemaphoreType.DMA
    vmem = pl.BlockSpec(memory_space=pltpu.VMEM)
    full = jax.ShapeDtypeStruct(orbitals.shape, f32)
    return pl.pallas_call(
        functools.partial(body, cols),
        out_shape=(full, full),
        in_specs=[vmem] * 2 + [pl.BlockSpec(memory_space=pl.ANY)] * 4,
        out_specs=(vmem, vmem),
        scratch_shapes=[
            *[pltpu.VMEM(a.shape, a.dtype) for a in consts],
            pltpu.VMEM((cols, 2, 2, 2, 2, SENT, PLANE), bf16),
            pltpu.VMEM((2, 2, HX, PLANE), f32),
            pltpu.VMEM((2, HX, PLANE), f32),
            pltpu.VMEM((cols, 2, 2, 2, HX, PLANE), f32),
            pltpu.VMEM((2, n, LANES), f32),
            pltpu.VMEM((2, n), f32),
            pltpu.VMEM((2, n_orb, 2, n), f32),
            pltpu.VMEM((n, n), f32),
            dma((4,)),
            dma,
            dma,
            dma((3, cols)),
            dma((3, cols)),
            dma((3, cols, 2)),
            dma((3, cols, 2, 2)),
            dma((2,)),
            dma((2,)),
            dma((2 * n_orb,)),
            dma((2, n_orb)),
            dma((2, cols)),
            dma((2, cols)),
            dma((2, cols, 2)),
            dma((2, cols, 2, 2)),
        ],
        compiler_params=pltpu.CompilerParams(
            collective_id=0, has_side_effects=True, vmem_limit_bytes=60 * 1024 * 1024
        ),
        name="exchange",
    )(orbitals, occupation[None], *consts)


def solution(mesh):
    return jax.shard_map(
        on_device,
        mesh=mesh,
        in_specs=(P("orb", "grid"), P("orb")),
        out_specs=(P("orb", "grid"), P("orb", "grid")),
        check_vma=False,
    )
```

```python
import functools
import math

import jax
import jax.numpy as jnp
import numpy as np
from jax import lax
from jax.experimental import pallas as pl
from jax.experimental.pallas import tpu as pltpu
from jax.sharding import PartitionSpec as P

NX = 20
NY = 24
NZ = 24
NPTS = NX * NY * NZ
PLANE = NY * NZ
HALVES = 2
HX = NX // HALVES
TILE = 8
EDGE = HX - TILE
ROWS = 3 * TILE
LANES = 128
BATCH = 8
MESH = pl.DeviceIdType.MESH


def hartley_table(length):
    index = np.arange(length, dtype=np.int32)
    product = index[:, None] * index[None, :] % length
    angle = np.float32(2.0 * math.pi / length) * product.astype(np.float32)
    return np.cos(angle) + np.sin(angle)


def signed_square(length):
    index = np.arange(length, dtype=np.int32)
    signed = np.where(index <= length // 2, index, index - length).astype(np.float32)
    return (np.float32(2.0 * math.pi) * signed / np.float32(length)) ** 2


def padded_rows(array):
    zero = np.zeros((TILE - 2 * EDGE,) + array.shape[1:], array.dtype)
    first, second = array[:HX], array[HX:]
    parts = [first[:TILE], first[TILE:], second[TILE:], zero, second[:TILE]]
    return np.concatenate(parts, axis=0)


def tables():
    table_x = padded_rows(padded_rows(hartley_table(NX)).T)
    table_x = np.kron(np.eye(BATCH, dtype=np.float32), table_x)
    table_y = np.kron(hartley_table(NY), np.eye(NZ, dtype=np.float32))
    table_z = np.kron(np.eye(16, dtype=np.float32), hartley_table(NZ))
    total = (
        signed_square(NX)[:, None, None]
        + signed_square(NY)[None, :, None]
        + signed_square(NZ)[None, None, :]
    )
    safe = np.where(total > 0, total, 1.0)
    kernel = np.where(total > 0, 1.0 / safe, 0.0) / NPTS
    kernel = padded_rows(kernel.reshape(NX, PLANE).astype(np.float32))
    return (
        jnp.asarray(table_x, jnp.bfloat16),
        jnp.asarray(table_y, jnp.bfloat16),
        jnp.asarray(table_z, jnp.bfloat16),
        jnp.asarray(kernel, jnp.float32),
    )


def column_of(matrix, k):
    if isinstance(k, int):
        return matrix[:, k : k + 1]
    lane = lax.broadcasted_iota(jnp.int32, matrix.shape, 1)
    return jnp.sum(jnp.where(lane == k, matrix, 0.0), axis=1, keepdims=True)


def row_of(matrix, k):
    if isinstance(k, int):
        return matrix[k : k + 1, :]
    line = lax.broadcasted_iota(jnp.int32, matrix.shape, 0)
    return jnp.sum(jnp.where(line == k, matrix, 0.0), axis=0, keepdims=True)


def loop(count, body, carry, most=64):
    if count <= most:
        for k in range(count):
            carry = body(k, carry)
        return carry
    return lax.fori_loop(0, count, body, carry)


def body(
    cols,
    own_ref,
    occ_ref,
    tx_hbm,
    ty_hbm,
    tz_hbm,
    k_hbm,
    pot_ref,
    proj_ref,
    tx_ref,
    ty_ref,
    tz_ref,
    k_ref,
    src,
    part,
    part_in,
    pots,
    pedge,
    edge_out,
    edge_in,
    rowsum,
    gown,
    gall,
    gmat,
    s_tab,
    s_x,
    r_x,
    s_a,
    s_y,
    s_c,
    r_in,
    s_p,
    r_p,
    s_g,
    r_g,
    t_a,
    t_y,
    t_c,
    t_in,
):
    o = lax.axis_index("orb")
    g = lax.axis_index("grid")
    n_orb = 4 * cols
    n = 2 * n_orb
    r = o // 4
    y = (o % 4) // 2
    c = o % 2
    h = 1 - g
    f32 = jnp.float32
    bf16 = jnp.bfloat16
    o_y = r * 4 + (1 - y) * 2 + c
    o_c = r * 4 + y * 2 + (1 - c)

    loads = [
        pltpu.make_async_copy(a, b, s_tab.at[i])
        for i, (a, b) in enumerate(
            ((tx_hbm, tx_ref), (ty_hbm, ty_ref), (tz_hbm, tz_ref), (k_hbm, k_ref))
        )
    ]
    for load in loads:
        load.start()

    barrier = pltpu.get_barrier_semaphore()

    def greet(orb, grid):
        pl.semaphore_signal(barrier, inc=1, device_id=(orb, grid), device_id_type=MESH)

    @pl.loop(1, cols)
    def _(d):
        greet((r + d) % cols * 4 + y * 2 + c, g)

    greet(o, h)
    greet(o_y, g)
    greet(o_c, g)

    own = own_ref[...].astype(f32)
    occ = occ_ref[...].astype(f32)
    own_edges = []
    for t in range(2):
        lines = [own[t : t + 1, PLANE * x : PLANE * (x + 1)] for x in range(HX)]
        src[r, y, c, t, 2 * g] = jnp.concatenate(lines[:TILE], axis=0).astype(bf16)
        own_edges += lines[TILE:]
    own_edges = jnp.concatenate(own_edges + [jnp.zeros((2 * EDGE, PLANE), f32)], axis=0)
    edge_out[...] = own_edges.astype(bf16)

    pl.semaphore_wait(barrier, cols + 2)

    def copy(source, target, send, recv, orb, grid):
        return pltpu.make_async_remote_copy(
            src_ref=source,
            dst_ref=target,
            send_sem=send,
            recv_sem=recv,
            device_id=(orb, grid),
            device_id_type=MESH,
        )

    def piece(j, q, u, w):
        if j == 0:
            return src.at[q, u, w, g, 2 * g]
        if j == 1:
            return src.at[q, u, w, g, pl.ds(h, 2)]
        return src.at[q, u, w, h, pl.ds(g, 2)]

    def same(ref, send, recv, orb):
        return copy(ref, ref, send, recv, orb, g)

    def to_column(j, d):
        q = (r + d) % cols
        return same(piece(j, r, y, c), s_a.at[j, q], r_in.at[j, r, y, c], q * 4 + y * 2 + c)

    def to_y(j, q):
        return same(piece(j, q, y, c), s_y.at[j, q], r_in.at[j, q, y, c], o_y)

    def to_core(j, q, u):
        return same(piece(j, q, u, c), s_c.at[j, q, u], r_in.at[j, q, u, c], o_c)

    def arrived(j, q, u, w):
        same(piece(j, q, u, w), s_a.at[j, r], r_in.at[j, q, u, w], o_c).wait_recv()

    def crossing(half):
        tile = src.at[r, y, c, :, 2 * half]
        return copy(tile, tile, s_x.at[0], r_x.at[0], o, h)

    crosses = (crossing(g), copy(edge_out, edge_in, s_x.at[1], r_x.at[1], o, h))
    for cross in crosses:
        cross.start()

    def send_own(j):
        @pl.loop(1, cols)
        def _(d):
            to_column(j, cols - d).start()

        to_y(j, r).start()
        to_core(j, r, y).start()

    send_own(0)
    crossing(h).wait_recv()
    crosses[1].wait_recv()
    second_half = g.astype(f32)
    first_half = 1.0 - second_half
    edges = edge_in[...].astype(f32)
    low = own_edges * first_half + edges * second_half
    high = edges * first_half + own_edges * second_half
    for t in range(2):
        own_lines = slice(EDGE * t, EDGE * (t + 1))
        lines = [low[own_lines], high[own_lines]]
        lines.append(jnp.broadcast_to(occ[:, t : t + 1], (1, PLANE)))
        lines.append(jnp.zeros((TILE - 2 * EDGE - 1, PLANE), f32))
        src[r, y, c, t, 1] = jnp.concatenate(lines, axis=0).astype(bf16)
    send_own(1)

    def relay_column(j):
        @pl.loop(1, cols)
        def _(d):
            q = (r + d) % cols
            arrived(j, q, y, c)
            to_y(j, q).start()
            to_core(j, q, y).start()

    def relay_y(j):
        @pl.loop(0, cols)
        def _(d):
            q = (r + d) % cols
            arrived(j, q, 1 - y, c)
            to_core(j, q, 1 - y).start()

    def other_core(j, u):
        @pl.loop(0, cols)
        def _(q):
            arrived(j, q, u, 1 - c)

    relay_column(0)
    relay_column(1)
    send_own(2)
    for load in loads:
        load.wait()
    other_core(0, y)
    other_core(1, y)

    tx = tx_ref[...]
    ty = ty_ref[...]
    tz = tz_ref[...]
    cut = tz.shape[0]
    rest = PLANE - cut
    kern = k_ref[...]

    def mm(a, b):
        return jnp.dot(a, b, preferred_element_type=f32)

    def along_z(a):
        return jnp.concatenate([mm(a[:, :cut], tz), mm(a[:, cut:], tz[:rest, :rest])], axis=1)

    per = BATCH // 2
    block = (BATCH, ROWS, PLANE)
    flat_block = (BATCH * ROWS, PLANE)
    steps = cols // per

    def one_batch(u, step, t, first):
        raw = src[pl.ds(step * per, per), u, :, g].reshape(BATCH * 3, TILE, PLANE)
        raw = raw.astype(f32).reshape(block)
        weight = raw[:, TILE + 2 * EDGE : TILE + 2 * EDGE + 1, :]
        target = src[r, y, c, t].astype(f32).reshape(block[1:])
        density = (raw * target[None]).reshape(flat_block).astype(bf16)
        s = mm(tx, density).astype(bf16)
        s = mm(s, ty).astype(bf16)
        s = along_z(s).reshape(block) * kern[None]
        s = along_z(s.reshape(flat_block).astype(bf16)).astype(bf16)
        s = mm(s, ty).astype(bf16)
        v = mm(tx, s).reshape(block)
        total = jnp.sum(weight * v * raw, axis=0).reshape(3, TILE, PLANE)
        if first:
            part[t] = -total
        else:
            part[t] -= total

    def batches(u, t, first):
        if first:
            one_batch(u, 0, t, True)
        if steps > int(first):

            @pl.loop(int(first), steps)
            def _(k):
                one_batch(u, k, t, False)

    batches(y, 0, True)
    relay_y(0)
    relay_y(1)
    batches(y, 1, True)
    relay_column(2)
    other_core(0, 1 - y)
    other_core(1, 1 - y)
    batches(1 - y, 0, False)

    def swap(t):
        return copy(part.at[t, pl.ds(h, 2)], part_in.at[t], s_p.at[t], r_p.at[t], o, h)

    swap(0).start()
    batches(1 - y, 1, False)
    swap(1).start()

    relay_y(2)

    def pot_at(t, q, u, w):
        return pedge.at[q, u, w] if t == 2 else pots.at[q, u, w, t]

    def pot_column(t, d):
        q = (r + d) % cols
        return same(pot_at(t, r, y, c), t_a.at[t, q], t_in.at[t, r, y, c], q * 4 + y * 2 + c)

    def pot_y(t, q):
        return same(pot_at(t, q, y, c), t_y.at[t, q], t_in.at[t, q, y, c], o_y)

    def pot_core(t, q, u):
        return same(pot_at(t, q, u, c), t_c.at[t, q, u], t_in.at[t, q, u, c], o_c)

    def pot_arrived(t, q, u, w):
        same(pot_at(t, q, u, w), t_a.at[t, r], t_in.at[t, q, u, w], o_c).wait_recv()

    def send_pots(t):
        @pl.loop(1, cols)
        def _(d):
            pot_column(t, cols - d).start()

        pot_y(t, r).start()
        pot_core(t, r, y).start()

    def gram_rows(t, value):
        @pl.loop(0, cols)
        def _(q):
            rows = src[q, :, :, :, 2 * g].reshape(8, TILE, PLANE).astype(f32)
            ends = src[q, :, :, :, 1].reshape(8, TILE, PLANE).astype(f32)
            sums = jnp.sum(rows * value[0][None] + ends * value[2][None], axis=1)
            fold = sums[:, :LANES]
            for k in range(LANES, PLANE - LANES + 1, LANES):
                fold += sums[:, k : k + LANES]
            tail = PLANE % LANES
            if tail:
                last = jnp.zeros((8, LANES - tail), f32)
                fold += jnp.concatenate([sums[:, PLANE - tail :], last], axis=1)
            rowsum[t, pl.ds(pl.multiple_of(q * 8, 8), 8), :] = fold

        ones = jnp.ones((8, LANES), f32)
        sums = lax.dot_general(
            ones,
            rowsum[t],
            (((1,), (1,)), ((), ())),
            precision=lax.Precision.HIGHEST,
            preferred_element_type=f32,
        )
        gown[t : t + 1, :] = sums[0:1]

    def finish(t):
        swap(t).wait_recv()
        tile = part[t, 2 * g] + part_in[t, g]
        pots[r, y, c, t] = tile
        rest = part[t, 1] + part_in[t, h]
        edge = rest[:EDGE] * first_half + rest[EDGE : 2 * EDGE] * second_half
        line = lax.broadcasted_iota(jnp.int32, (TILE, PLANE), 0)
        return tile, edge, jnp.where(line // EDGE == g, rest, 0.0)

    value0 = finish(0)
    send_pots(0)
    other_core(2, y)
    other_core(2, 1 - y)
    gram_rows(0, value0)
    value1 = finish(1)
    gram_rows(1, value1)
    gall[g, o] = gown[...]

    def gram_to(d):
        flat = (o * 2 + g + d) % (2 * n_orb)
        return copy(gown, gall.at[g, o], s_g.at[d], r_g.at[g, o], flat // 2, flat % 2)

    @pl.loop(1, 2 * n_orb)
    def _(d):
        gram_to(d).start()

    pedge[r, y, c] = jnp.concatenate([value0[1], value1[1]], axis=0)
    send_pots(1)
    send_pots(2)

    def write(ref, t, value):
        for x in range(0, HX, 2):
            pair = jnp.concatenate([value[x : x + 1], value[x + 1 : x + 2]], axis=1)
            ref[t : t + 1, PLANE * x : PLANE * (x + 2)] = pair

    write(pot_ref, 0, jnp.concatenate(value0[:2], axis=0))
    write(pot_ref, 1, jnp.concatenate(value1[:2], axis=0))

    def pot_relay_column(t):
        @pl.loop(1, cols)
        def _(d):
            q = (r + d) % cols
            pot_arrived(t, q, y, c)
            pot_y(t, q).start()
            pot_core(t, q, y).start()

    def pot_relay_y(t):
        @pl.loop(0, cols)
        def _(d):
            q = (r + d) % cols
            pot_arrived(t, q, 1 - y, c)
            pot_core(t, q, 1 - y).start()

    pot_relay_column(0)
    pot_relay_column(1)
    pot_relay_column(2)
    pot_relay_y(0)

    for cross in crosses:
        cross.wait_send()
    for t in range(2):
        swap(t).wait_send()

    @pl.loop(1, cols)
    def _(d):
        for j in range(3):
            to_column(j, d).wait_send()

    @pl.loop(0, cols)
    def _(q):
        for j in range(3):
            to_y(j, q).wait_send()
            for u in range(2):
                to_core(j, q, u).wait_send()

    @pl.loop(1, 2 * n_orb)
    def _(d):
        flat = (o * 2 + g + d) % (2 * n_orb)
        there = gall.at[flat % 2, flat // 2]
        copy(there, there, s_g.at[0], r_g.at[flat % 2, flat // 2], o_c, g).wait_recv()

    def assemble(k, carry):
        pairs = [gall[0, 4 * k + j] + gall[1, 4 * k + j] for j in range(4)]
        start = 8 * k if isinstance(k, int) else pl.multiple_of(8 * k, 8)
        gmat[pl.ds(start, 8), :] = jnp.concatenate(pairs, axis=0)
        return carry

    loop(cols, assemble, 0, 16)
    gram = gmat[...]
    sym = (gram + gram.T) * f32(-0.5 / NPTS)
    row_id = lax.broadcasted_iota(jnp.int32, (n, n), 0)
    eye = (row_id == lax.broadcasted_iota(jnp.int32, (n, n), 1)).astype(f32)
    below = lax.broadcasted_iota(jnp.int32, (n, 1), 0)

    def eliminate(k, pair):
        left, right = pair
        row_l = row_of(left, k)
        scale = 1.0 / column_of(row_l, k)
        factor = jnp.where(below > k, column_of(left, k) * scale, 0.0)
        return left - factor * row_l, right - factor * row_of(right, k)

    early = n * 3 // 4
    if n <= 64:
        pair = loop(early, eliminate, (sym, eye))
        pot_relay_y(1)
        pot_relay_y(2)
        for k in range(early, n):
            pair = eliminate(k, pair)
        left, right = pair
    else:
        pot_relay_y(1)
        pot_relay_y(2)
        left, right = loop(n, eliminate, (sym, eye))
    diag = jnp.sum(left * eye, axis=1, keepdims=True)
    inverse = right * (1.0 / jnp.sqrt(diag))
    a0, a1 = row_of(inverse, 2 * o), row_of(inverse, 2 * o + 1)

    @pl.loop(0, cols)
    def _(q):
        for u in range(2):
            for t in range(3):
                pot_arrived(t, q, u, 1 - c)

    def add(k, sums):
        where = (k // 4, k % 4 // 2, k % 2)
        if not isinstance(k, int):
            where = (k // 4, lax.rem(k, 4) // 2, lax.rem(k, 2))
        edge = pedge[where]
        tiles = [pots[where + (t,)] for t in range(2)]
        ends = [edge[EDGE * t : EDGE * (t + 1)] for t in range(2)]
        new = []
        for a, (tile, end) in zip((a0, a1), sums):
            for t in range(2):
                factor = column_of(a, 2 * k + t)
                tile, end = tile + factor * tiles[t], end + factor * ends[t]
            new.append((tile, end))
        return tuple(new)

    zero = (jnp.zeros((TILE, PLANE), f32), jnp.zeros((EDGE, PLANE), f32))
    proj = loop(n_orb, add, (zero, zero))
    for t in range(2):
        write(proj_ref, t, jnp.concatenate(proj[t], axis=0))

    @pl.loop(1, cols)
    def _(d):
        for t in range(3):
            pot_column(t, d).wait_send()

    @pl.loop(0, cols)
    def _(q):
        for t in range(3):
            pot_y(t, q).wait_send()
            for u in range(2):
                pot_core(t, q, u).wait_send()

    @pl.loop(1, 2 * n_orb)
    def _(d):
        gram_to(d).wait_send()


def on_device(orbitals, occupation):
    n_orb = lax.axis_size("orb")
    cols = n_orb // 4
    n = 2 * n_orb
    consts = tables()
    f32 = jnp.float32
    bf16 = jnp.bfloat16
    dma = pltpu.SemaphoreType.DMA
    vmem = pl.BlockSpec(memory_space=pltpu.VMEM)
    full = jax.ShapeDtypeStruct(orbitals.shape, f32)
    return pl.pallas_call(
        functools.partial(body, cols),
        out_shape=(full, full),
        in_specs=[vmem] * 2 + [pl.BlockSpec(memory_space=pl.ANY)] * 4,
        out_specs=(vmem, vmem),
        scratch_shapes=[
            *[pltpu.VMEM(a.shape, a.dtype) for a in consts],
            pltpu.VMEM((cols, 2, 2, 2, 3, TILE, PLANE), bf16),
            pltpu.VMEM((2, 3, TILE, PLANE), f32),
            pltpu.VMEM((2, 2, TILE, PLANE), f32),
            pltpu.VMEM((cols, 2, 2, 2, TILE, PLANE), f32),
            pltpu.VMEM((cols, 2, 2, 2 * EDGE, PLANE), f32),
            pltpu.VMEM((TILE, PLANE), bf16),
            pltpu.VMEM((TILE, PLANE), bf16),
            pltpu.VMEM((2, n, LANES), f32),
            pltpu.VMEM((2, n), f32),
            pltpu.VMEM((2, n_orb, 2, n), f32),
            pltpu.VMEM((n, n), f32),
            dma((4,)),
            dma((2,)),
            dma((2,)),
            dma((3, cols)),
            dma((3, cols)),
            dma((3, cols, 2)),
            dma((3, cols, 2, 2)),
            dma((2,)),
            dma((2,)),
            dma((2 * n_orb,)),
            dma((2, n_orb)),
            dma((3, cols)),
            dma((3, cols)),
            dma((3, cols, 2)),
            dma((3, cols, 2, 2)),
        ],
        compiler_params=pltpu.CompilerParams(
            collective_id=0, has_side_effects=True, vmem_limit_bytes=60 * 1024 * 1024
        ),
        name="exchange",
    )(orbitals, occupation[None], *consts)


def solution(mesh):
    return jax.shard_map(
        on_device,
        mesh=mesh,
        in_specs=(P("orb", "grid"), P("orb")),
        out_specs=(P("orb", "grid"), P("orb", "grid")),
        check_vma=False,
    )
```

```python
import functools
import math

import jax
import jax.numpy as jnp
import numpy as np
from jax import lax
from jax.experimental import pallas as pl
from jax.experimental.pallas import tpu as pltpu
from jax.sharding import PartitionSpec as P

NX = 20
NY = 24
NZ = 24
NPTS = NX * NY * NZ
PLANE = NY * NZ
HALVES = 2
HX = NX // HALVES
TILE = 8
EDGE = HX - TILE
ROWS = 3 * TILE
LANES = 128
BATCH = 8
MESH = pl.DeviceIdType.MESH


def hartley_table(length):
    index = np.arange(length, dtype=np.int32)
    product = index[:, None] * index[None, :] % length
    angle = np.float32(2.0 * math.pi / length) * product.astype(np.float32)
    return np.cos(angle) + np.sin(angle)


def signed_square(length):
    index = np.arange(length, dtype=np.int32)
    signed = np.where(index <= length // 2, index, index - length).astype(np.float32)
    return (np.float32(2.0 * math.pi) * signed / np.float32(length)) ** 2


def padded_rows(array):
    zero = np.zeros((TILE - 2 * EDGE,) + array.shape[1:], array.dtype)
    first, second = array[:HX], array[HX:]
    parts = [first[:TILE], first[TILE:], second[TILE:], zero, second[:TILE]]
    return np.concatenate(parts, axis=0)


def tables():
    table_x = padded_rows(padded_rows(hartley_table(NX)).T)
    table_x = np.kron(np.eye(BATCH, dtype=np.float32), table_x)
    table_y = np.kron(hartley_table(NY), np.eye(NZ, dtype=np.float32))
    table_z = np.kron(np.eye(16, dtype=np.float32), hartley_table(NZ))
    total = (
        signed_square(NX)[:, None, None]
        + signed_square(NY)[None, :, None]
        + signed_square(NZ)[None, None, :]
    )
    safe = np.where(total > 0, total, 1.0)
    kernel = np.where(total > 0, 1.0 / safe, 0.0) / NPTS
    kernel = padded_rows(kernel.reshape(NX, PLANE).astype(np.float32))
    return (
        jnp.asarray(table_x, jnp.bfloat16),
        jnp.asarray(table_y, jnp.bfloat16),
        jnp.asarray(table_z, jnp.bfloat16),
        jnp.asarray(kernel, jnp.float32),
    )


def column_of(matrix, k):
    if isinstance(k, int):
        return matrix[:, k : k + 1]
    lane = lax.broadcasted_iota(jnp.int32, matrix.shape, 1)
    return jnp.sum(jnp.where(lane == k, matrix, 0.0), axis=1, keepdims=True)


def row_of(matrix, k):
    if isinstance(k, int):
        return matrix[k : k + 1, :]
    line = lax.broadcasted_iota(jnp.int32, matrix.shape, 0)
    return jnp.sum(jnp.where(line == k, matrix, 0.0), axis=0, keepdims=True)


def loop(count, body, carry, most=64):
    if count <= most:
        for k in range(count):
            carry = body(k, carry)
        return carry
    return lax.fori_loop(0, count, body, carry)


def body(
    cols,
    own_ref,
    occ_ref,
    tx_hbm,
    ty_hbm,
    tz_hbm,
    k_hbm,
    pot_out,
    proj_out,
    pot_ref,
    proj_ref,
    s_o,
    tx_ref,
    ty_ref,
    tz_ref,
    k_ref,
    src,
    part,
    part_in,
    pots,
    pedge,
    edge_out,
    edge_in,
    rowsum,
    gown,
    gall,
    gmat,
    s_tab,
    s_x,
    r_x,
    s_a,
    s_y,
    s_c,
    r_col,
    r_y,
    r_core,
    s_p,
    r_p,
    s_g,
    r_g,
    t_a,
    t_y,
    t_c,
    t_col,
    t_yin,
    t_core,
):
    o = lax.axis_index("orb")
    g = lax.axis_index("grid")
    n_orb = 4 * cols
    n = 2 * n_orb
    r = o // 4
    y = (o % 4) // 2
    c = o % 2
    h = 1 - g
    f32 = jnp.float32
    bf16 = jnp.bfloat16
    o_y = r * 4 + (1 - y) * 2 + c
    o_c = r * 4 + y * 2 + (1 - c)

    loads = [
        pltpu.make_async_copy(a, b, s_tab.at[i])
        for i, (a, b) in enumerate(
            ((tx_hbm, tx_ref), (ty_hbm, ty_ref), (tz_hbm, tz_ref), (k_hbm, k_ref))
        )
    ]
    for load in loads:
        load.start()

    barrier = pltpu.get_barrier_semaphore()

    def greet(orb, grid):
        pl.semaphore_signal(barrier, inc=1, device_id=(orb, grid), device_id_type=MESH)

    @pl.loop(1, cols)
    def _(d):
        greet((r + d) % cols * 4 + y * 2 + c, g)

    greet(o, h)
    greet(o_y, g)
    greet(o_c, g)

    own = own_ref[...].astype(f32)
    occ = occ_ref[...].astype(f32)
    own_edges = []
    for t in range(2):
        lines = [own[t : t + 1, PLANE * x : PLANE * (x + 1)] for x in range(HX)]
        src[r, y, c, t, 2 * g] = jnp.concatenate(lines[:TILE], axis=0).astype(bf16)
        own_edges += lines[TILE:]
    own_edges = jnp.concatenate(own_edges + [jnp.zeros((2 * EDGE, PLANE), f32)], axis=0)
    edge_out[...] = own_edges.astype(bf16)

    pl.semaphore_wait(barrier, cols + 2)

    def copy(source, target, send, recv, orb, grid):
        return pltpu.make_async_remote_copy(
            src_ref=source,
            dst_ref=target,
            send_sem=send,
            recv_sem=recv,
            device_id=(orb, grid),
            device_id_type=MESH,
        )

    def piece(j, q, u, w):
        if j == 0:
            return src.at[q, u, w, g, 2 * g]
        if j == 1:
            return src.at[q, u, w, g, pl.ds(h, 2)]
        return src.at[q, u, w, h, pl.ds(g, 2)]

    def same(ref, send, recv, orb):
        return copy(ref, ref, send, recv, orb, g)

    def to_column(j, d):
        q = (r + d) % cols
        return same(piece(j, r, y, c), s_a.at[j], r_col.at[j, r], q * 4 + y * 2 + c)

    def to_y(j, q):
        return same(piece(j, q, y, c), s_y.at[j], r_y.at[j, q], o_y)

    def to_core(j, q, u):
        return same(piece(j, q, u, c), s_c.at[j], r_core.at[j, u], o_c)

    def arrived(j, q, u, w, recv):
        same(piece(j, q, u, w), s_a.at[j], recv, o_c).wait_recv()

    everyone = pl.ds(0, cols)
    others = pl.ds(0, cols - 1)
    both = pl.ds(0, 2)

    def crossing(half):
        tile = src.at[r, y, c, :, 2 * half]
        return copy(tile, tile, s_x.at[0], r_x.at[0], o, h)

    crosses = (crossing(g), copy(edge_out, edge_in, s_x.at[1], r_x.at[1], o, h))
    for cross in crosses:
        cross.start()

    def send_own(j):
        @pl.loop(1, cols)
        def _(d):
            to_column(j, cols - d).start()

        to_y(j, r).start()
        to_core(j, r, y).start()

    send_own(0)
    crossing(h).wait_recv()
    crosses[1].wait_recv()
    second_half = g.astype(f32)
    first_half = 1.0 - second_half
    edges = edge_in[...].astype(f32)
    low = own_edges * first_half + edges * second_half
    high = edges * first_half + own_edges * second_half
    for t in range(2):
        own_lines = slice(EDGE * t, EDGE * (t + 1))
        lines = [low[own_lines], high[own_lines]]
        lines.append(jnp.broadcast_to(occ[:, t : t + 1], (1, PLANE)))
        lines.append(jnp.zeros((TILE - 2 * EDGE - 1, PLANE), f32))
        src[r, y, c, t, 1] = jnp.concatenate(lines, axis=0).astype(bf16)
    send_own(1)

    def relay_column(j):
        @pl.loop(1, cols)
        def _(d):
            q = (r + d) % cols
            arrived(j, q, y, c, r_col.at[j, q])
            to_y(j, q).start()
            to_core(j, q, y).start()

    def relay_y(j):
        @pl.loop(0, cols)
        def _(d):
            q = (r + d) % cols
            arrived(j, q, 1 - y, c, r_y.at[j, q])
            to_core(j, q, 1 - y).start()

    def other_core(j, u):
        arrived(j, everyone, u, 1 - c, r_core.at[j, u])

    relay_column(0)
    relay_column(1)
    send_own(2)
    for load in loads:
        load.wait()
    other_core(0, y)
    other_core(1, y)

    tx = tx_ref[...]
    ty = ty_ref[...]
    tz = tz_ref[...]
    cut = tz.shape[0]
    rest = PLANE - cut
    kern = k_ref[...]

    def mm(a, b):
        return jnp.dot(a, b, preferred_element_type=f32)

    def along_z(a):
        return jnp.concatenate([mm(a[:, :cut], tz), mm(a[:, cut:], tz[:rest, :rest])], axis=1)

    per = BATCH // 2
    block = (BATCH, ROWS, PLANE)
    flat_block = (BATCH * ROWS, PLANE)
    steps = cols // per

    def one_batch(u, step, t, first):
        raw = src[pl.ds(step * per, per), u, :, g].reshape(BATCH * 3, TILE, PLANE)
        raw = raw.astype(f32).reshape(block)
        weight = raw[:, TILE + 2 * EDGE : TILE + 2 * EDGE + 1, :]
        target = src[r, y, c, t].astype(f32).reshape(block[1:])
        density = (raw * target[None]).reshape(flat_block).astype(bf16)
        s = mm(tx, density).astype(bf16)
        s = mm(s, ty).astype(bf16)
        s = along_z(s).reshape(block) * kern[None]
        s = along_z(s.reshape(flat_block).astype(bf16)).astype(bf16)
        s = mm(s, ty).astype(bf16)
        v = mm(tx, s).reshape(block)
        total = jnp.sum(weight * v * raw, axis=0).reshape(3, TILE, PLANE)
        if first:
            part[t] = -total
        else:
            part[t] -= total

    def batches(u, t, first):
        if first:
            one_batch(u, 0, t, True)
        if steps > int(first):

            @pl.loop(int(first), steps)
            def _(k):
                one_batch(u, k, t, False)

    batches(y, 0, True)
    relay_y(0)
    relay_y(1)
    batches(y, 1, True)
    relay_column(2)
    other_core(0, 1 - y)
    other_core(1, 1 - y)
    batches(1 - y, 0, False)

    def swap(t):
        return copy(part.at[t, pl.ds(h, 2)], part_in.at[t], s_p.at[t], r_p.at[t], o, h)

    swap(0).start()
    batches(1 - y, 1, False)
    swap(1).start()

    relay_y(2)

    def pot_at(t, q, u, w):
        return pedge.at[q, u, w] if t == 2 else pots.at[q, u, w, t]

    def pot_column(t, d):
        q = (r + d) % cols
        return same(pot_at(t, r, y, c), t_a.at[t], t_col.at[t, r], q * 4 + y * 2 + c)

    def pot_y(t, q):
        return same(pot_at(t, q, y, c), t_y.at[t], t_yin.at[t, q], o_y)

    def pot_core(t, q, u):
        return same(pot_at(t, q, u, c), t_c.at[t], t_core.at[t, u], o_c)

    def pot_arrived(t, q, u, w, recv):
        same(pot_at(t, q, u, w), t_a.at[t], recv, o_c).wait_recv()

    def send_pots(t):
        @pl.loop(1, cols)
        def _(d):
            pot_column(t, cols - d).start()

        pot_y(t, r).start()
        pot_core(t, r, y).start()

    def gram_rows(t, value):
        @pl.loop(0, cols)
        def _(q):
            rows = src[q, :, :, :, 2 * g].reshape(8, TILE, PLANE).astype(f32)
            ends = src[q, :, :, :, 1].reshape(8, TILE, PLANE).astype(f32)
            sums = jnp.sum(rows * value[0][None] + ends * value[2][None], axis=1)
            fold = sums[:, :LANES]
            for k in range(LANES, PLANE - LANES + 1, LANES):
                fold += sums[:, k : k + LANES]
            tail = PLANE % LANES
            if tail:
                last = jnp.zeros((8, LANES - tail), f32)
                fold += jnp.concatenate([sums[:, PLANE - tail :], last], axis=1)
            rowsum[t, pl.ds(pl.multiple_of(q * 8, 8), 8), :] = fold

        ones = jnp.ones((8, LANES), f32)
        sums = lax.dot_general(
            ones,
            rowsum[t],
            (((1,), (1,)), ((), ())),
            precision=lax.Precision.HIGHEST,
            preferred_element_type=f32,
        )
        gown[t : t + 1, :] = sums[0:1]

    def finish(t):
        swap(t).wait_recv()
        tile = part[t, 2 * g] + part_in[t, g]
        pots[r, y, c, t] = tile
        rest = part[t, 1] + part_in[t, h]
        edge = rest[:EDGE] * first_half + rest[EDGE : 2 * EDGE] * second_half
        line = lax.broadcasted_iota(jnp.int32, (TILE, PLANE), 0)
        return tile, edge, jnp.where(line // EDGE == g, rest, 0.0)

    value0 = finish(0)
    send_pots(0)
    other_core(2, y)
    other_core(2, 1 - y)
    gram_rows(0, value0)
    value1 = finish(1)
    gram_rows(1, value1)
    gall[g * n_orb + o] = gown[...]

    def gram_to(d):
        flat = (o * 2 + g + d) % (2 * n_orb)
        return copy(gown, gall.at[g * n_orb + o], s_g, r_g, flat // 2, flat % 2)

    @pl.loop(1, 2 * n_orb)
    def _(d):
        gram_to(d).start()

    pedge[r, y, c] = jnp.concatenate([value0[1], value1[1]], axis=0)
    send_pots(1)
    send_pots(2)

    def write(ref, t, value):
        for x in range(0, HX, 2):
            pair = jnp.concatenate([value[x : x + 1], value[x + 1 : x + 2]], axis=1)
            ref[t : t + 1, PLANE * x : PLANE * (x + 2)] = pair

    write(pot_ref, 0, jnp.concatenate(value0[:2], axis=0))
    write(pot_ref, 1, jnp.concatenate(value1[:2], axis=0))
    store_pot = pltpu.make_async_copy(pot_ref, pot_out, s_o.at[0])
    store_pot.start()

    def pot_relay_column(t):
        @pl.loop(1, cols)
        def _(d):
            q = (r + d) % cols
            pot_arrived(t, q, y, c, t_col.at[t, q])
            pot_y(t, q).start()
            pot_core(t, q, y).start()

    def pot_relay_y(t):
        @pl.loop(0, cols)
        def _(d):
            q = (r + d) % cols
            pot_arrived(t, q, 1 - y, c, t_yin.at[t, q])
            pot_core(t, q, 1 - y).start()

    pot_relay_column(0)
    pot_relay_column(1)
    pot_relay_column(2)
    pot_relay_y(0)

    for cross in crosses:
        cross.wait_send()
    for t in range(2):
        swap(t).wait_send()

    for j in range(3):
        same(piece(j, others, y, c), s_a.at[j], r_col.at[j, r], o_c).wait_send()
        same(piece(j, everyone, y, c), s_y.at[j], r_col.at[j, r], o_c).wait_send()
        same(piece(j, everyone, both, c), s_c.at[j], r_col.at[j, r], o_c).wait_send()

    received = gall.at[pl.ds(0, 2 * n_orb - 1)]
    grams = copy(received, received, s_g, r_g, o_c, g)
    grams.wait_recv()

    def assemble(k, carry):
        pairs = [gall[4 * k + j] + gall[n_orb + 4 * k + j] for j in range(4)]
        start = 8 * k if isinstance(k, int) else pl.multiple_of(8 * k, 8)
        gmat[pl.ds(start, 8), :] = jnp.concatenate(pairs, axis=0)
        return carry

    loop(cols, assemble, 0, 16)
    gram = gmat[...]
    sym = (gram + gram.T) * f32(-0.5 / NPTS)
    row_id = lax.broadcasted_iota(jnp.int32, (n, n), 0)
    eye = (row_id == lax.broadcasted_iota(jnp.int32, (n, n), 1)).astype(f32)
    below = lax.broadcasted_iota(jnp.int32, (n, 1), 0)

    def eliminate(k, pair):
        left, right = pair
        row_l = row_of(left, k)
        scale = 1.0 / column_of(row_l, k)
        factor = jnp.where(below > k, column_of(left, k) * scale, 0.0)
        return left - factor * row_l, right - factor * row_of(right, k)

    early = n * 3 // 4
    if n <= 64:
        pair = loop(early, eliminate, (sym, eye))
        pot_relay_y(1)
        pot_relay_y(2)
        for k in range(early, n):
            pair = eliminate(k, pair)
        left, right = pair
    else:
        pot_relay_y(1)
        pot_relay_y(2)
        left, right = loop(n, eliminate, (sym, eye))
    diag = jnp.sum(left * eye, axis=1, keepdims=True)
    inverse = right * (1.0 / jnp.sqrt(diag))
    a0, a1 = row_of(inverse, 2 * o), row_of(inverse, 2 * o + 1)

    for u in range(2):
        for t in range(3):
            pot_arrived(t, everyone, u, 1 - c, t_core.at[t, u])

    def add(k, sums):
        where = (k // 4, k % 4 // 2, k % 2)
        if not isinstance(k, int):
            where = (k // 4, lax.rem(k, 4) // 2, lax.rem(k, 2))
        edge = pedge[where]
        tiles = [pots[where + (t,)] for t in range(2)]
        ends = [edge[EDGE * t : EDGE * (t + 1)] for t in range(2)]
        new = []
        for a, (tile, end) in zip((a0, a1), sums):
            for t in range(2):
                factor = column_of(a, 2 * k + t)
                tile, end = tile + factor * tiles[t], end + factor * ends[t]
            new.append((tile, end))
        return tuple(new)

    zero = (jnp.zeros((TILE, PLANE), f32), jnp.zeros((EDGE, PLANE), f32))
    proj = loop(n_orb, add, (zero, zero))
    for t in range(2):
        write(proj_ref, t, jnp.concatenate(proj[t], axis=0))
    store_proj = pltpu.make_async_copy(proj_ref, proj_out, s_o.at[1])
    store_proj.start()

    for t in range(3):
        same(pot_at(t, others, y, c), t_a.at[t], t_col.at[t, r], o_c).wait_send()
        same(pot_at(t, everyone, y, c), t_y.at[t], t_col.at[t, r], o_c).wait_send()
        same(pot_at(t, everyone, both, c), t_c.at[t], t_col.at[t, r], o_c).wait_send()

    grams.wait_send()

    store_pot.wait()
    store_proj.wait()


def on_device(orbitals, occupation):
    n_orb = lax.axis_size("orb")
    cols = n_orb // 4
    n = 2 * n_orb
    consts = tables()
    f32 = jnp.float32
    bf16 = jnp.bfloat16
    dma = pltpu.SemaphoreType.DMA
    vmem = pl.BlockSpec(memory_space=pltpu.VMEM)
    full = jax.ShapeDtypeStruct(orbitals.shape, f32)
    return pl.pallas_call(
        functools.partial(body, cols),
        out_shape=(full, full),
        in_specs=[vmem] * 2 + [pl.BlockSpec(memory_space=pl.ANY)] * 4,
        out_specs=(pl.BlockSpec(memory_space=pl.ANY),) * 2,
        scratch_shapes=[
            pltpu.VMEM(orbitals.shape, f32),
            pltpu.VMEM(orbitals.shape, f32),
            dma((2,)),
            *[pltpu.VMEM(a.shape, a.dtype) for a in consts],
            pltpu.VMEM((cols, 2, 2, 2, 3, TILE, PLANE), bf16),
            pltpu.VMEM((2, 3, TILE, PLANE), f32),
            pltpu.VMEM((2, 2, TILE, PLANE), f32),
            pltpu.VMEM((cols, 2, 2, 2, TILE, PLANE), f32),
            pltpu.VMEM((cols, 2, 2, 2 * EDGE, PLANE), f32),
            pltpu.VMEM((TILE, PLANE), bf16),
            pltpu.VMEM((TILE, PLANE), bf16),
            pltpu.VMEM((2, n, LANES), f32),
            pltpu.VMEM((2, n), f32),
            pltpu.VMEM((2 * n_orb, 2, n), f32),
            pltpu.VMEM((n, n), f32),
            dma((4,)),
            dma((2,)),
            dma((2,)),
            dma((3,)),
            dma((3,)),
            dma((3,)),
            dma((3, cols)),
            dma((3, cols)),
            dma((3, 2)),
            dma((2,)),
            dma((2,)),
            dma,
            dma,
            dma((3,)),
            dma((3,)),
            dma((3,)),
            dma((3, cols)),
            dma((3, cols)),
            dma((3, 2)),
        ],
        compiler_params=pltpu.CompilerParams(
            collective_id=0, has_side_effects=True, vmem_limit_bytes=60 * 1024 * 1024
        ),
        name="exchange",
    )(orbitals, occupation[None], *consts)


def solution(mesh):
    return jax.shard_map(
        on_device,
        mesh=mesh,
        in_specs=(P("orb", "grid"), P("orb")),
        out_specs=(P("orb", "grid"), P("orb", "grid")),
        check_vma=False,
    )
```

```python
import functools
import math

import jax
import jax.numpy as jnp
import numpy as np
from jax import lax
from jax.experimental import pallas as pl
from jax.experimental.pallas import tpu as pltpu
from jax.sharding import PartitionSpec as P

NX = 20
NY = 24
NZ = 24
NPTS = NX * NY * NZ
PLANE = NY * NZ
HALVES = 2
HX = NX // HALVES
TILE = 8
EDGE = HX - TILE
ROWS = 3 * TILE
LANES = 128
BATCH = 8
MESH = pl.DeviceIdType.MESH


def hartley_table(length):
    index = np.arange(length, dtype=np.int32)
    product = index[:, None] * index[None, :] % length
    angle = np.float32(2.0 * math.pi / length) * product.astype(np.float32)
    return np.cos(angle) + np.sin(angle)


def signed_square(length):
    index = np.arange(length, dtype=np.int32)
    signed = np.where(index <= length // 2, index, index - length).astype(np.float32)
    return (np.float32(2.0 * math.pi) * signed / np.float32(length)) ** 2


def padded_rows(array):
    zero = np.zeros((TILE - 2 * EDGE,) + array.shape[1:], array.dtype)
    first, second = array[:HX], array[HX:]
    parts = [first[:TILE], first[TILE:], second[TILE:], zero, second[:TILE]]
    return np.concatenate(parts, axis=0)


def tables():
    table_x = padded_rows(padded_rows(hartley_table(NX)).T)
    table_x = np.kron(np.eye(BATCH, dtype=np.float32), table_x)
    table_y = np.kron(hartley_table(NY), np.eye(NZ, dtype=np.float32))
    table_z = np.kron(np.eye(16, dtype=np.float32), hartley_table(NZ))
    total = (
        signed_square(NX)[:, None, None]
        + signed_square(NY)[None, :, None]
        + signed_square(NZ)[None, None, :]
    )
    safe = np.where(total > 0, total, 1.0)
    kernel = np.where(total > 0, 1.0 / safe, 0.0) / NPTS
    kernel = padded_rows(kernel.reshape(NX, PLANE).astype(np.float32))
    return (
        jnp.asarray(table_x, jnp.bfloat16),
        jnp.asarray(table_y, jnp.bfloat16),
        jnp.asarray(table_z, jnp.bfloat16),
        jnp.asarray(kernel, jnp.float32),
    )


def column_of(matrix, k):
    if isinstance(k, int):
        return matrix[:, k : k + 1]
    lane = lax.broadcasted_iota(jnp.int32, matrix.shape, 1)
    return jnp.sum(jnp.where(lane == k, matrix, 0.0), axis=1, keepdims=True)


def row_of(matrix, k):
    if isinstance(k, int):
        return matrix[k : k + 1, :]
    line = lax.broadcasted_iota(jnp.int32, matrix.shape, 0)
    return jnp.sum(jnp.where(line == k, matrix, 0.0), axis=0, keepdims=True)


def loop(count, body, carry, most=64):
    if count <= most:
        for k in range(count):
            carry = body(k, carry)
        return carry
    return lax.fori_loop(0, count, body, carry)


def body(
    cols,
    own_ref,
    occ_ref,
    tx_hbm,
    ty_hbm,
    tz_hbm,
    k_hbm,
    pot_out,
    proj_out,
    pot_ref,
    proj_ref,
    s_o,
    tx_ref,
    ty_ref,
    tz_ref,
    k_ref,
    src,
    part,
    part_in,
    pots,
    pedge,
    edge_out,
    edge_in,
    rowsum,
    gown,
    gall,
    gmat,
    s_tab,
    s_x,
    r_x,
    s_a,
    s_y,
    s_c,
    r_col,
    r_y,
    r_core,
    s_p,
    r_p,
    s_g,
    r_g,
    t_a,
    t_y,
    t_c,
    t_col,
    t_yin,
    t_core,
):
    o = lax.axis_index("orb")
    g = lax.axis_index("grid")
    n_orb = 4 * cols
    n = 2 * n_orb
    r = o // 4
    y = (o % 4) // 2
    c = o % 2
    h = 1 - g
    f32 = jnp.float32
    bf16 = jnp.bfloat16
    o_y = r * 4 + (1 - y) * 2 + c
    o_c = r * 4 + y * 2 + (1 - c)

    loads = [
        pltpu.make_async_copy(a, b, s_tab.at[i])
        for i, (a, b) in enumerate(
            ((tx_hbm, tx_ref), (ty_hbm, ty_ref), (tz_hbm, tz_ref), (k_hbm, k_ref))
        )
    ]
    for load in loads:
        load.start()

    barrier = pltpu.get_barrier_semaphore()

    def greet(orb, grid):
        pl.semaphore_signal(barrier, inc=1, device_id=(orb, grid), device_id_type=MESH)

    @pl.loop(1, cols)
    def _(d):
        greet((r + d) % cols * 4 + y * 2 + c, g)

    greet(o, h)
    greet(o_y, g)
    greet(o_c, g)

    own = own_ref[...].astype(f32)
    occ = occ_ref[...].astype(f32)
    own_edges = []
    for t in range(2):
        lines = [own[t : t + 1, PLANE * x : PLANE * (x + 1)] for x in range(HX)]
        src[r, y, c, t, 2 * g] = jnp.concatenate(lines[:TILE], axis=0).astype(bf16)
        own_edges += lines[TILE:]
    own_edges = jnp.concatenate(own_edges + [jnp.zeros((2 * EDGE, PLANE), f32)], axis=0)
    edge_out[...] = own_edges.astype(bf16)

    pl.semaphore_wait(barrier, cols + 2)

    def copy(source, target, send, recv, orb, grid):
        return pltpu.make_async_remote_copy(
            src_ref=source,
            dst_ref=target,
            send_sem=send,
            recv_sem=recv,
            device_id=(orb, grid),
            device_id_type=MESH,
        )

    def piece(j, q, u, w):
        if j == 0:
            return src.at[q, u, w, g, 2 * g]
        if j == 1:
            return src.at[q, u, w, g, pl.ds(h, 2)]
        return src.at[q, u, w, h, pl.ds(g, 2)]

    def same(ref, send, recv, orb):
        return copy(ref, ref, send, recv, orb, g)

    def to_column(j, d):
        q = (r + d) % cols
        return same(piece(j, r, y, c), s_a.at[j], r_col.at[j, r], q * 4 + y * 2 + c)

    def to_y(j, q):
        return same(piece(j, q, y, c), s_y.at[j], r_y.at[j, q], o_y)

    def to_core(j, q, u):
        return same(piece(j, q, u, c), s_c.at[j], r_core.at[j, u], o_c)

    def arrived(j, q, u, w, recv):
        same(piece(j, q, u, w), s_a.at[j], recv, o_c).wait_recv()

    everyone = pl.ds(0, cols)
    others = pl.ds(0, cols - 1)
    both = pl.ds(0, 2)

    def crossing(half):
        tile = src.at[r, y, c, :, 2 * half]
        return copy(tile, tile, s_x.at[0], r_x.at[0], o, h)

    crosses = (crossing(g), copy(edge_out, edge_in, s_x.at[1], r_x.at[1], o, h))
    for cross in crosses:
        cross.start()

    def send_own(j):
        @pl.loop(1, cols)
        def _(d):
            to_column(j, cols - d).start()

        to_y(j, r).start()
        to_core(j, r, y).start()

    send_own(0)
    crossing(h).wait_recv()
    crosses[1].wait_recv()
    second_half = g.astype(f32)
    first_half = 1.0 - second_half
    edges = edge_in[...].astype(f32)
    low = own_edges * first_half + edges * second_half
    high = edges * first_half + own_edges * second_half
    for t in range(2):
        own_lines = slice(EDGE * t, EDGE * (t + 1))
        lines = [low[own_lines], high[own_lines]]
        lines.append(jnp.broadcast_to(occ[:, t : t + 1], (1, PLANE)))
        lines.append(jnp.zeros((TILE - 2 * EDGE - 1, PLANE), f32))
        src[r, y, c, t, 1] = jnp.concatenate(lines, axis=0).astype(bf16)
    send_own(1)

    def relay_column(j):
        @pl.loop(1, cols)
        def _(d):
            q = (r + d) % cols
            arrived(j, q, y, c, r_col.at[j, q])
            to_y(j, q).start()
            to_core(j, q, y).start()

    def relay_y(j):
        @pl.loop(0, cols)
        def _(d):
            q = (r + d) % cols
            arrived(j, q, 1 - y, c, r_y.at[j, q])
            to_core(j, q, 1 - y).start()

    def other_core(j, u):
        arrived(j, everyone, u, 1 - c, r_core.at[j, u])

    relay_column(0)
    relay_column(1)
    send_own(2)
    for load in loads:
        load.wait()
    other_core(0, y)
    other_core(1, y)

    tx = tx_ref[...]
    ty = ty_ref[...]
    tz = tz_ref[...]
    cut = tz.shape[0]
    rest = PLANE - cut
    kern = k_ref[...]

    def mm(a, b):
        return jnp.dot(a, b, preferred_element_type=f32)

    def along_z(a):
        return jnp.concatenate([mm(a[:, :cut], tz), mm(a[:, cut:], tz[:rest, :rest])], axis=1)

    per = BATCH // 2
    block = (BATCH, ROWS, PLANE)
    flat_block = (BATCH * ROWS, PLANE)
    steps = cols // per

    def one_batch(u, step, t, first):
        raw = src[pl.ds(step * per, per), u, :, g].reshape(BATCH * 3, TILE, PLANE)
        raw = raw.astype(f32).reshape(block)
        weight = raw[:, TILE + 2 * EDGE : TILE + 2 * EDGE + 1, :]
        target = src[r, y, c, t].astype(f32).reshape(block[1:])
        density = (raw * target[None]).reshape(flat_block).astype(bf16)
        s = mm(tx, density).astype(bf16)
        s = mm(s, ty).astype(bf16)
        s = along_z(s).reshape(block) * kern[None]
        s = along_z(s.reshape(flat_block).astype(bf16)).astype(bf16)
        s = mm(s, ty).astype(bf16)
        v = mm(tx, s).reshape(block)
        total = jnp.sum(weight * v * raw, axis=0).reshape(3, TILE, PLANE)
        if first:
            part[t] = -total
        else:
            part[t] -= total

    def batches(u, t, first):
        if first:
            one_batch(u, 0, t, True)
        if steps > int(first):

            @pl.loop(int(first), steps)
            def _(k):
                one_batch(u, k, t, False)

    batches(y, 0, True)
    relay_y(0)
    relay_y(1)
    batches(y, 1, True)
    relay_column(2)
    other_core(0, 1 - y)
    other_core(1, 1 - y)
    batches(1 - y, 0, False)

    def swap(t):
        return copy(part.at[t, pl.ds(h, 2)], part_in.at[t], s_p.at[t], r_p.at[t], o, h)

    swap(0).start()
    batches(1 - y, 1, False)
    swap(1).start()

    relay_y(2)

    def pot_at(t, q, u, w):
        return pedge.at[q, u, w] if t == 2 else pots.at[q, u, w, t]

    def pot_column(t, d):
        q = (r + d) % cols
        return same(pot_at(t, r, y, c), t_a.at[t], t_col.at[t, r], q * 4 + y * 2 + c)

    def pot_y(t, q):
        return same(pot_at(t, q, y, c), t_y.at[t], t_yin.at[t, q], o_y)

    def pot_core(t, q, u):
        return same(pot_at(t, q, u, c), t_c.at[t], t_core.at[t, u], o_c)

    def pot_arrived(t, q, u, w, recv):
        same(pot_at(t, q, u, w), t_a.at[t], recv, o_c).wait_recv()

    def send_pots(t):
        @pl.loop(1, cols)
        def _(d):
            pot_column(t, cols - d).start()

        pot_y(t, r).start()
        pot_core(t, r, y).start()

    def gram_rows(t, value):
        @pl.loop(0, cols)
        def _(q):
            rows = src[q, :, :, :, 2 * g].reshape(8, TILE, PLANE).astype(f32)
            ends = src[q, :, :, :, 1].reshape(8, TILE, PLANE).astype(f32)
            sums = jnp.sum(rows * value[0][None] + ends * value[2][None], axis=1)
            fold = sums[:, :LANES]
            for k in range(LANES, PLANE - LANES + 1, LANES):
                fold += sums[:, k : k + LANES]
            tail = PLANE % LANES
            if tail:
                last = jnp.zeros((8, LANES - tail), f32)
                fold += jnp.concatenate([sums[:, PLANE - tail :], last], axis=1)
            rowsum[t, pl.ds(pl.multiple_of(q * 8, 8), 8), :] = fold

        gown[t : t + 1, :] = jnp.sum(rowsum[t].T, axis=0, keepdims=True)

    def finish(t):
        swap(t).wait_recv()
        tile = part[t, 2 * g] + part_in[t, g]
        pots[r, y, c, t] = tile
        rest = part[t, 1] + part_in[t, h]
        edge = rest[:EDGE] * first_half + rest[EDGE : 2 * EDGE] * second_half
        line = lax.broadcasted_iota(jnp.int32, (TILE, PLANE), 0)
        return tile, edge, jnp.where(line // EDGE == g, rest, 0.0)

    value0 = finish(0)
    send_pots(0)
    other_core(2, y)
    other_core(2, 1 - y)
    gram_rows(0, value0)
    value1 = finish(1)
    gram_rows(1, value1)
    gall[g * n_orb + o] = gown[...]

    def gram_to(d):
        flat = (o * 2 + g + d) % (2 * n_orb)
        return copy(gown, gall.at[g * n_orb + o], s_g, r_g, flat // 2, flat % 2)

    @pl.loop(1, 2 * n_orb)
    def _(d):
        gram_to(d).start()

    pedge[r, y, c] = jnp.concatenate([value0[1], value1[1]], axis=0)
    send_pots(1)
    send_pots(2)

    def write(ref, t, value):
        for x in range(0, HX, 2):
            pair = jnp.concatenate([value[x : x + 1], value[x + 1 : x + 2]], axis=1)
            ref[t : t + 1, PLANE * x : PLANE * (x + 2)] = pair

    write(pot_ref, 0, jnp.concatenate(value0[:2], axis=0))
    write(pot_ref, 1, jnp.concatenate(value1[:2], axis=0))
    store_pot = pltpu.make_async_copy(pot_ref, pot_out, s_o.at[0])
    store_pot.start()

    def pot_relay_column(t):
        @pl.loop(1, cols)
        def _(d):
            q = (r + d) % cols
            pot_arrived(t, q, y, c, t_col.at[t, q])
            pot_y(t, q).start()
            pot_core(t, q, y).start()

    def pot_relay_y(t):
        @pl.loop(0, cols)
        def _(d):
            q = (r + d) % cols
            pot_arrived(t, q, 1 - y, c, t_yin.at[t, q])
            pot_core(t, q, 1 - y).start()

    pot_relay_column(0)
    pot_relay_column(1)
    pot_relay_column(2)
    pot_relay_y(0)

    for cross in crosses:
        cross.wait_send()
    for t in range(2):
        swap(t).wait_send()

    for j in range(3):
        same(piece(j, others, y, c), s_a.at[j], r_col.at[j, r], o_c).wait_send()
        same(piece(j, everyone, y, c), s_y.at[j], r_col.at[j, r], o_c).wait_send()
        same(piece(j, everyone, both, c), s_c.at[j], r_col.at[j, r], o_c).wait_send()

    received = gall.at[pl.ds(0, 2 * n_orb - 1)]
    grams = copy(received, received, s_g, r_g, o_c, g)
    grams.wait_recv()

    def assemble(k, carry):
        pairs = [gall[4 * k + j] + gall[n_orb + 4 * k + j] for j in range(4)]
        start = 8 * k if isinstance(k, int) else pl.multiple_of(8 * k, 8)
        gmat[pl.ds(start, 8), :] = jnp.concatenate(pairs, axis=0)
        return carry

    loop(cols, assemble, 0, 16)
    gram = gmat[...]
    sym = (gram + gram.T) * f32(-0.5 / NPTS)
    row_id = lax.broadcasted_iota(jnp.int32, (n, n), 0)
    eye = (row_id == lax.broadcasted_iota(jnp.int32, (n, n), 1)).astype(f32)
    below = lax.broadcasted_iota(jnp.int32, (n, 1), 0)

    def eliminate(k, pair):
        left, right = pair
        row_l = row_of(left, k)
        scale = 1.0 / column_of(row_l, k)
        factor = jnp.where(below > k, column_of(left, k) * scale, 0.0)
        return left - factor * row_l, right - factor * row_of(right, k)

    early = n * 3 // 4
    if n <= 64:
        pair = loop(early, eliminate, (sym, eye))
        pot_relay_y(1)
        pot_relay_y(2)
        for k in range(early, n):
            pair = eliminate(k, pair)
        left, right = pair
    else:
        pot_relay_y(1)
        pot_relay_y(2)
        left, right = loop(n, eliminate, (sym, eye))
    diag = jnp.sum(left * eye, axis=1, keepdims=True)
    inverse = right * (1.0 / jnp.sqrt(diag))
    a0, a1 = row_of(inverse, 2 * o), row_of(inverse, 2 * o + 1)

    for u in range(2):
        for t in range(3):
            pot_arrived(t, everyone, u, 1 - c, t_core.at[t, u])

    def add(k, sums):
        where = (k // 4, k % 4 // 2, k % 2)
        if not isinstance(k, int):
            where = (k // 4, lax.rem(k, 4) // 2, lax.rem(k, 2))
        edge = pedge[where]
        tiles = [pots[where + (t,)] for t in range(2)]
        ends = [edge[EDGE * t : EDGE * (t + 1)] for t in range(2)]
        new = []
        for a, (tile, end) in zip((a0, a1), sums):
            for t in range(2):
                factor = column_of(a, 2 * k + t)
                tile, end = tile + factor * tiles[t], end + factor * ends[t]
            new.append((tile, end))
        return tuple(new)

    zero = (jnp.zeros((TILE, PLANE), f32), jnp.zeros((EDGE, PLANE), f32))
    proj = loop(n_orb, add, (zero, zero))
    for t in range(2):
        write(proj_ref, t, jnp.concatenate(proj[t], axis=0))
    store_proj = pltpu.make_async_copy(proj_ref, proj_out, s_o.at[1])
    store_proj.start()

    for t in range(3):
        same(pot_at(t, others, y, c), t_a.at[t], t_col.at[t, r], o_c).wait_send()
        same(pot_at(t, everyone, y, c), t_y.at[t], t_col.at[t, r], o_c).wait_send()
        same(pot_at(t, everyone, both, c), t_c.at[t], t_col.at[t, r], o_c).wait_send()

    grams.wait_send()

    store_pot.wait()
    store_proj.wait()


def on_device(orbitals, occupation):
    n_orb = lax.axis_size("orb")
    cols = n_orb // 4
    n = 2 * n_orb
    consts = tables()
    f32 = jnp.float32
    bf16 = jnp.bfloat16
    dma = pltpu.SemaphoreType.DMA
    vmem = pl.BlockSpec(memory_space=pltpu.VMEM)
    full = jax.ShapeDtypeStruct(orbitals.shape, f32)
    return pl.pallas_call(
        functools.partial(body, cols),
        out_shape=(full, full),
        in_specs=[vmem] * 2 + [pl.BlockSpec(memory_space=pl.ANY)] * 4,
        out_specs=(pl.BlockSpec(memory_space=pl.ANY),) * 2,
        scratch_shapes=[
            pltpu.VMEM(orbitals.shape, f32),
            pltpu.VMEM(orbitals.shape, f32),
            dma((2,)),
            *[pltpu.VMEM(a.shape, a.dtype) for a in consts],
            pltpu.VMEM((cols, 2, 2, 2, 3, TILE, PLANE), bf16),
            pltpu.VMEM((2, 3, TILE, PLANE), f32),
            pltpu.VMEM((2, 2, TILE, PLANE), f32),
            pltpu.VMEM((cols, 2, 2, 2, TILE, PLANE), f32),
            pltpu.VMEM((cols, 2, 2, 2 * EDGE, PLANE), f32),
            pltpu.VMEM((TILE, PLANE), bf16),
            pltpu.VMEM((TILE, PLANE), bf16),
            pltpu.VMEM((2, n, LANES), f32),
            pltpu.VMEM((2, n), f32),
            pltpu.VMEM((2 * n_orb, 2, n), f32),
            pltpu.VMEM((n, n), f32),
            dma((4,)),
            dma((2,)),
            dma((2,)),
            dma((3,)),
            dma((3,)),
            dma((3,)),
            dma((3, cols)),
            dma((3, cols)),
            dma((3, 2)),
            dma((2,)),
            dma((2,)),
            dma,
            dma,
            dma((3,)),
            dma((3,)),
            dma((3,)),
            dma((3, cols)),
            dma((3, cols)),
            dma((3, 2)),
        ],
        compiler_params=pltpu.CompilerParams(
            collective_id=0, has_side_effects=True, vmem_limit_bytes=60 * 1024 * 1024
        ),
        name="exchange",
    )(orbitals, occupation[None], *consts)


def solution(mesh):
    return jax.shard_map(
        on_device,
        mesh=mesh,
        in_specs=(P("orb", "grid"), P("orb")),
        out_specs=(P("orb", "grid"), P("orb", "grid")),
        check_vma=False,
    )
```

```python
import functools
import math

import jax
import jax.numpy as jnp
import numpy as np
from jax import lax
from jax.experimental import pallas as pl
from jax.experimental.pallas import tpu as pltpu
from jax.sharding import PartitionSpec as P

NX = 20
NY = 24
NZ = 24
NPTS = NX * NY * NZ
PLANE = NY * NZ
HALVES = 2
HX = NX // HALVES
TILE = 8
EDGE = HX - TILE
ROWS = 3 * TILE
LANES = 128
BATCH = 8
MESH = pl.DeviceIdType.MESH


def hartley_table(length):
    index = np.arange(length, dtype=np.int32)
    product = index[:, None] * index[None, :] % length
    angle = np.float32(2.0 * math.pi / length) * product.astype(np.float32)
    return np.cos(angle) + np.sin(angle)


def signed_square(length):
    index = np.arange(length, dtype=np.int32)
    signed = np.where(index <= length // 2, index, index - length).astype(np.float32)
    return (np.float32(2.0 * math.pi) * signed / np.float32(length)) ** 2


def padded_rows(array):
    zero = np.zeros((TILE - 2 * EDGE,) + array.shape[1:], array.dtype)
    first, second = array[:HX], array[HX:]
    parts = [first[:TILE], first[TILE:], second[TILE:], zero, second[:TILE]]
    return np.concatenate(parts, axis=0)


def tables():
    table_x = padded_rows(padded_rows(hartley_table(NX)).T)
    table_x = np.kron(np.eye(BATCH, dtype=np.float32), table_x)
    table_y = np.kron(hartley_table(NY), np.eye(NZ, dtype=np.float32))
    table_z = np.kron(np.eye(16, dtype=np.float32), hartley_table(NZ))
    total = (
        signed_square(NX)[:, None, None]
        + signed_square(NY)[None, :, None]
        + signed_square(NZ)[None, None, :]
    )
    safe = np.where(total > 0, total, 1.0)
    kernel = np.where(total > 0, 1.0 / safe, 0.0) / NPTS
    kernel = padded_rows(kernel.reshape(NX, PLANE).astype(np.float32))
    return (
        jnp.asarray(table_x, jnp.bfloat16),
        jnp.asarray(table_y, jnp.bfloat16),
        jnp.asarray(table_z, jnp.bfloat16),
        jnp.asarray(kernel, jnp.float32),
    )


def column_of(matrix, k):
    if isinstance(k, int):
        return matrix[:, k : k + 1]
    lane = lax.broadcasted_iota(jnp.int32, matrix.shape, 1)
    return jnp.sum(jnp.where(lane == k, matrix, 0.0), axis=1, keepdims=True)


def row_of(matrix, k):
    if isinstance(k, int):
        return matrix[k : k + 1, :]
    line = lax.broadcasted_iota(jnp.int32, matrix.shape, 0)
    return jnp.sum(jnp.where(line == k, matrix, 0.0), axis=0, keepdims=True)


def loop(count, body, carry, most=64):
    if count <= most:
        for k in range(count):
            carry = body(k, carry)
        return carry
    return lax.fori_loop(0, count, body, carry)


def body(
    cols,
    own_ref,
    occ_ref,
    tx_hbm,
    ty_hbm,
    tz_hbm,
    k_hbm,
    pot_out,
    proj_out,
    pot_ref,
    proj_ref,
    s_o,
    tx_ref,
    ty_ref,
    tz_ref,
    k_ref,
    src,
    part,
    part_in,
    pots,
    pedge,
    edge_out,
    edge_in,
    rowsum,
    gown,
    gall,
    gmat,
    s_tab,
    s_x,
    r_x,
    s_a,
    s_y,
    s_c,
    r_col,
    r_y,
    r_core,
    s_p,
    r_p,
    s_g,
    r_g,
    t_a,
    t_y,
    t_c,
    t_col,
    t_yin,
    t_core,
):
    o = lax.axis_index("orb")
    g = lax.axis_index("grid")
    n_orb = 4 * cols
    n = 2 * n_orb
    r = o // 4
    y = (o % 4) // 2
    c = o % 2
    h = 1 - g
    f32 = jnp.float32
    bf16 = jnp.bfloat16
    o_y = r * 4 + (1 - y) * 2 + c
    o_c = r * 4 + y * 2 + (1 - c)

    loads = [
        pltpu.make_async_copy(a, b, s_tab.at[i])
        for i, (a, b) in enumerate(
            ((tx_hbm, tx_ref), (ty_hbm, ty_ref), (tz_hbm, tz_ref), (k_hbm, k_ref))
        )
    ]
    for load in loads:
        load.start()

    barrier = pltpu.get_barrier_semaphore()

    def greet(orb, grid):
        pl.semaphore_signal(barrier, inc=1, device_id=(orb, grid), device_id_type=MESH)

    @pl.loop(1, cols)
    def _(d):
        greet((r + d) % cols * 4 + y * 2 + c, g)

    greet(o, h)
    greet(o_y, g)
    greet(o_c, g)

    own = own_ref[...].astype(f32)
    occ = occ_ref[...].astype(f32)
    own_edges = []
    for t in range(2):
        lines = [own[t : t + 1, PLANE * x : PLANE * (x + 1)] for x in range(HX)]
        src[r, y, c, t, 2 * g] = jnp.concatenate(lines[:TILE], axis=0).astype(bf16)
        own_edges += lines[TILE:]
    own_edges = jnp.concatenate(own_edges + [jnp.zeros((2 * EDGE, PLANE), f32)], axis=0)
    edge_out[...] = own_edges.astype(bf16)

    pl.semaphore_wait(barrier, cols + 2)

    def copy(source, target, send, recv, orb, grid):
        return pltpu.make_async_remote_copy(
            src_ref=source,
            dst_ref=target,
            send_sem=send,
            recv_sem=recv,
            device_id=(orb, grid),
            device_id_type=MESH,
        )

    def piece(j, q, u, w):
        if j == 0:
            return src.at[q, u, w, g, 2 * g]
        if j == 1:
            return src.at[q, u, w, g, pl.ds(h, 2)]
        return src.at[q, u, w, h, pl.ds(g, 2)]

    def same(ref, send, recv, orb):
        return copy(ref, ref, send, recv, orb, g)

    def to_column(j, d):
        q = (r + d) % cols
        return same(piece(j, r, y, c), s_a.at[j], r_col.at[j, r], q * 4 + y * 2 + c)

    def to_y(j, q):
        return same(piece(j, q, y, c), s_y.at[j], r_y.at[j, q], o_y)

    def to_core(j, q, u):
        return same(piece(j, q, u, c), s_c.at[j], r_core.at[j, u], o_c)

    def arrived(j, q, u, w, recv):
        same(piece(j, q, u, w), s_a.at[j], recv, o_c).wait_recv()

    everyone = pl.ds(0, cols)
    others = pl.ds(0, cols - 1)
    both = pl.ds(0, 2)

    def crossing(half):
        tile = src.at[r, y, c, :, 2 * half]
        return copy(tile, tile, s_x.at[0], r_x.at[0], o, h)

    crosses = (crossing(g), copy(edge_out, edge_in, s_x.at[1], r_x.at[1], o, h))
    for cross in crosses:
        cross.start()

    def send_own(j):
        @pl.loop(1, cols)
        def _(d):
            to_column(j, cols - d).start()

        to_y(j, r).start()
        to_core(j, r, y).start()

    send_own(0)
    crossing(h).wait_recv()
    crosses[1].wait_recv()
    second_half = g.astype(f32)
    first_half = 1.0 - second_half
    edges = edge_in[...].astype(f32)
    low = own_edges * first_half + edges * second_half
    high = edges * first_half + own_edges * second_half
    for t in range(2):
        own_lines = slice(EDGE * t, EDGE * (t + 1))
        lines = [low[own_lines], high[own_lines]]
        lines.append(jnp.broadcast_to(occ[:, t : t + 1], (1, PLANE)))
        lines.append(jnp.zeros((TILE - 2 * EDGE - 1, PLANE), f32))
        src[r, y, c, t, 1] = jnp.concatenate(lines, axis=0).astype(bf16)
    send_own(1)

    def relay_column(j):
        @pl.loop(1, cols)
        def _(d):
            q = (r + d) % cols
            arrived(j, q, y, c, r_col.at[j, q])
            to_y(j, q).start()
            to_core(j, q, y).start()

    def relay_y(j):
        @pl.loop(0, cols)
        def _(d):
            q = (r + d) % cols
            arrived(j, q, 1 - y, c, r_y.at[j, q])
            to_core(j, q, 1 - y).start()

    def other_core(j, u):
        arrived(j, everyone, u, 1 - c, r_core.at[j, u])

    relay_column(0)
    relay_column(1)
    send_own(2)
    for load in loads:
        load.wait()
    other_core(0, y)
    other_core(1, y)

    tx = tx_ref[...]
    ty = ty_ref[...]
    tz = tz_ref[...]
    cut = tz.shape[0]
    rest = PLANE - cut
    kern = k_ref[...]

    def mm(a, b):
        return jnp.dot(a, b, preferred_element_type=f32)

    def along_z(a):
        return jnp.concatenate([mm(a[:, :cut], tz), mm(a[:, cut:], tz[:rest, :rest])], axis=1)

    per = BATCH // 2
    block = (BATCH, ROWS, PLANE)
    flat_block = (BATCH * ROWS, PLANE)
    steps = cols // per

    def one_batch(u, step, t, first):
        raw = src[pl.ds(step * per, per), u, :, g].reshape(BATCH * 3, TILE, PLANE)
        raw = raw.astype(f32).reshape(block)
        weight = raw[:, TILE + 2 * EDGE : TILE + 2 * EDGE + 1, :]
        target = src[r, y, c, t].astype(f32).reshape(block[1:])
        density = (raw * target[None]).reshape(flat_block).astype(bf16)
        s = mm(tx, density).astype(bf16)
        s = mm(s, ty).astype(bf16)
        s = along_z(s).reshape(block) * kern[None]
        s = along_z(s.reshape(flat_block).astype(bf16)).astype(bf16)
        s = mm(s, ty).astype(bf16)
        v = mm(tx, s).reshape(block)
        total = jnp.sum(weight * v * raw, axis=0).reshape(3, TILE, PLANE)
        if first:
            part[t] = -total
        else:
            part[t] -= total

    def batches(u, t, first):
        if first:
            one_batch(u, 0, t, True)
        if steps > int(first):

            @pl.loop(int(first), steps)
            def _(k):
                one_batch(u, k, t, False)

    batches(y, 0, True)
    relay_y(0)
    relay_y(1)
    batches(y, 1, True)
    relay_column(2)
    other_core(0, 1 - y)
    other_core(1, 1 - y)
    batches(1 - y, 0, False)

    def swap(t):
        return copy(part.at[t, pl.ds(h, 2)], part_in.at[t], s_p.at[t], r_p.at[t], o, h)

    swap(0).start()
    batches(1 - y, 1, False)
    swap(1).start()

    relay_y(2)

    def pot_at(t, q, u, w):
        return pedge.at[q, u, w] if t == 2 else pots.at[q, u, w, t]

    def pot_column(t, d):
        q = (r + d) % cols
        return same(pot_at(t, r, y, c), t_a.at[t], t_col.at[t, r], q * 4 + y * 2 + c)

    def pot_y(t, q):
        return same(pot_at(t, q, y, c), t_y.at[t], t_yin.at[t, q], o_y)

    def pot_core(t, q, u):
        return same(pot_at(t, q, u, c), t_c.at[t], t_core.at[t, u], o_c)

    def pot_arrived(t, q, u, w, recv):
        same(pot_at(t, q, u, w), t_a.at[t], recv, o_c).wait_recv()

    def send_pots(t):
        @pl.loop(1, cols)
        def _(d):
            pot_column(t, cols - d).start()

        pot_y(t, r).start()
        pot_core(t, r, y).start()

    def gram_rows(t, value):
        @pl.loop(0, cols)
        def _(q):
            rows = src[q, :, :, :, 2 * g].reshape(8, TILE, PLANE).astype(f32)
            ends = src[q, :, :, :, 1].reshape(8, TILE, PLANE).astype(f32)
            sums = jnp.sum(rows * value[0][None] + ends * value[2][None], axis=1)
            fold = sums[:, :LANES]
            for k in range(LANES, PLANE - LANES + 1, LANES):
                fold += sums[:, k : k + LANES]
            tail = PLANE % LANES
            if tail:
                last = jnp.zeros((8, LANES - tail), f32)
                fold += jnp.concatenate([sums[:, PLANE - tail :], last], axis=1)
            rowsum[t, pl.ds(pl.multiple_of(q * 8, 8), 8), :] = fold

        gown[t : t + 1, :] = jnp.sum(rowsum[t].T, axis=0, keepdims=True)

    def finish(t):
        swap(t).wait_recv()
        tile = part[t, 2 * g] + part_in[t, g]
        pots[r, y, c, t] = tile
        rest = part[t, 1] + part_in[t, h]
        edge = rest[:EDGE] * first_half + rest[EDGE : 2 * EDGE] * second_half
        line = lax.broadcasted_iota(jnp.int32, (TILE, PLANE), 0)
        return tile, edge, jnp.where(line // EDGE == g, rest, 0.0)

    value0 = finish(0)
    send_pots(0)
    other_core(2, y)
    other_core(2, 1 - y)
    gram_rows(0, value0)
    value1 = finish(1)
    send_pots(1)
    gram_rows(1, value1)
    gall[g * n_orb + o] = gown[...]

    def gram_to(d):
        flat = (o * 2 + g + d) % (2 * n_orb)
        return copy(gown, gall.at[g * n_orb + o], s_g, r_g, flat // 2, flat % 2)

    @pl.loop(1, 2 * n_orb)
    def _(d):
        gram_to(d).start()

    pedge[r, y, c] = jnp.concatenate([value0[1], value1[1]], axis=0)
    send_pots(2)

    def write(ref, t, value):
        for x in range(0, HX, 2):
            pair = jnp.concatenate([value[x : x + 1], value[x + 1 : x + 2]], axis=1)
            ref[t : t + 1, PLANE * x : PLANE * (x + 2)] = pair

    write(pot_ref, 0, jnp.concatenate(value0[:2], axis=0))
    write(pot_ref, 1, jnp.concatenate(value1[:2], axis=0))
    store_pot = pltpu.make_async_copy(pot_ref, pot_out, s_o.at[0])
    store_pot.start()

    def pot_relay_column(t):
        @pl.loop(1, cols)
        def _(d):
            q = (r + d) % cols
            pot_arrived(t, q, y, c, t_col.at[t, q])
            pot_y(t, q).start()
            pot_core(t, q, y).start()

    def pot_relay_y(t):
        @pl.loop(0, cols)
        def _(d):
            q = (r + d) % cols
            pot_arrived(t, q, 1 - y, c, t_yin.at[t, q])
            pot_core(t, q, 1 - y).start()

    pot_relay_column(0)
    pot_relay_column(1)
    pot_relay_column(2)
    pot_relay_y(0)

    for cross in crosses:
        cross.wait_send()
    for t in range(2):
        swap(t).wait_send()

    for j in range(3):
        same(piece(j, others, y, c), s_a.at[j], r_col.at[j, r], o_c).wait_send()
        same(piece(j, everyone, y, c), s_y.at[j], r_col.at[j, r], o_c).wait_send()
        same(piece(j, everyone, both, c), s_c.at[j], r_col.at[j, r], o_c).wait_send()

    received = gall.at[pl.ds(0, 2 * n_orb - 1)]
    grams = copy(received, received, s_g, r_g, o_c, g)
    grams.wait_recv()

    def assemble(k, carry):
        pairs = [gall[4 * k + j] + gall[n_orb + 4 * k + j] for j in range(4)]
        start = 8 * k if isinstance(k, int) else pl.multiple_of(8 * k, 8)
        gmat[pl.ds(start, 8), :] = jnp.concatenate(pairs, axis=0)
        return carry

    loop(cols, assemble, 0, 16)
    gram = gmat[...]
    sym = (gram + gram.T) * f32(-0.5 / NPTS)
    row_id = lax.broadcasted_iota(jnp.int32, (n, n), 0)
    eye = (row_id == lax.broadcasted_iota(jnp.int32, (n, n), 1)).astype(f32)
    below = lax.broadcasted_iota(jnp.int32, (n, 1), 0)

    def eliminate(k, pair):
        left, right = pair
        row_l = row_of(left, k)
        scale = 1.0 / column_of(row_l, k)
        factor = jnp.where(below > k, column_of(left, k) * scale, 0.0)
        return left - factor * row_l, right - factor * row_of(right, k)

    early = n * 3 // 4
    if n <= 64:
        pair = loop(early, eliminate, (sym, eye))
        pot_relay_y(1)
        pot_relay_y(2)
        for k in range(early, n):
            pair = eliminate(k, pair)
        left, right = pair
    else:
        pot_relay_y(1)
        pot_relay_y(2)
        left, right = loop(n, eliminate, (sym, eye))
    diag = jnp.sum(left * eye, axis=1, keepdims=True)
    inverse = right * (1.0 / jnp.sqrt(diag))
    a0, a1 = row_of(inverse, 2 * o), row_of(inverse, 2 * o + 1)

    for u in range(2):
        for t in range(3):
            pot_arrived(t, everyone, u, 1 - c, t_core.at[t, u])

    def add(k, sums):
        where = (k // 4, k % 4 // 2, k % 2)
        if not isinstance(k, int):
            where = (k // 4, lax.rem(k, 4) // 2, lax.rem(k, 2))
        edge = pedge[where]
        tiles = [pots[where + (t,)] for t in range(2)]
        ends = [edge[EDGE * t : EDGE * (t + 1)] for t in range(2)]
        new = []
        for a, (tile, end) in zip((a0, a1), sums):
            for t in range(2):
                factor = column_of(a, 2 * k + t)
                tile, end = tile + factor * tiles[t], end + factor * ends[t]
            new.append((tile, end))
        return tuple(new)

    zero = (jnp.zeros((TILE, PLANE), f32), jnp.zeros((EDGE, PLANE), f32))
    proj = loop(n_orb, add, (zero, zero))
    for t in range(2):
        write(proj_ref, t, jnp.concatenate(proj[t], axis=0))
    store_proj = pltpu.make_async_copy(proj_ref, proj_out, s_o.at[1])
    store_proj.start()

    for t in range(3):
        same(pot_at(t, others, y, c), t_a.at[t], t_col.at[t, r], o_c).wait_send()
        same(pot_at(t, everyone, y, c), t_y.at[t], t_col.at[t, r], o_c).wait_send()
        same(pot_at(t, everyone, both, c), t_c.at[t], t_col.at[t, r], o_c).wait_send()

    grams.wait_send()

    store_pot.wait()
    store_proj.wait()


def on_device(orbitals, occupation):
    n_orb = lax.axis_size("orb")
    cols = n_orb // 4
    n = 2 * n_orb
    consts = tables()
    f32 = jnp.float32
    bf16 = jnp.bfloat16
    dma = pltpu.SemaphoreType.DMA
    vmem = pl.BlockSpec(memory_space=pltpu.VMEM)
    full = jax.ShapeDtypeStruct(orbitals.shape, f32)
    return pl.pallas_call(
        functools.partial(body, cols),
        out_shape=(full, full),
        in_specs=[vmem] * 2 + [pl.BlockSpec(memory_space=pl.ANY)] * 4,
        out_specs=(pl.BlockSpec(memory_space=pl.ANY),) * 2,
        scratch_shapes=[
            pltpu.VMEM(orbitals.shape, f32),
            pltpu.VMEM(orbitals.shape, f32),
            dma((2,)),
            *[pltpu.VMEM(a.shape, a.dtype) for a in consts],
            pltpu.VMEM((cols, 2, 2, 2, 3, TILE, PLANE), bf16),
            pltpu.VMEM((2, 3, TILE, PLANE), f32),
            pltpu.VMEM((2, 2, TILE, PLANE), f32),
            pltpu.VMEM((cols, 2, 2, 2, TILE, PLANE), f32),
            pltpu.VMEM((cols, 2, 2, 2 * EDGE, PLANE), f32),
            pltpu.VMEM((TILE, PLANE), bf16),
            pltpu.VMEM((TILE, PLANE), bf16),
            pltpu.VMEM((2, n, LANES), f32),
            pltpu.VMEM((2, n), f32),
            pltpu.VMEM((2 * n_orb, 2, n), f32),
            pltpu.VMEM((n, n), f32),
            dma((4,)),
            dma((2,)),
            dma((2,)),
            dma((3,)),
            dma((3,)),
            dma((3,)),
            dma((3, cols)),
            dma((3, cols)),
            dma((3, 2)),
            dma((2,)),
            dma((2,)),
            dma,
            dma,
            dma((3,)),
            dma((3,)),
            dma((3,)),
            dma((3, cols)),
            dma((3, cols)),
            dma((3, 2)),
        ],
        compiler_params=pltpu.CompilerParams(
            collective_id=0, has_side_effects=True, vmem_limit_bytes=60 * 1024 * 1024
        ),
        name="exchange",
    )(orbitals, occupation[None], *consts)


def solution(mesh):
    return jax.shard_map(
        on_device,
        mesh=mesh,
        in_specs=(P("orb", "grid"), P("orb")),
        out_specs=(P("orb", "grid"), P("orb", "grid")),
        check_vma=False,
    )
```
